256 devices in a mesh: row: 8 (over y, x_hi), theta: 4 (over x_lo, core), gz: 8 (over z).
Axes of the slice: x: 4 (x_hi: 2, x_lo: 2; x = x_hi * 2 + x_lo), y: 4, z: 8, core: 2. Of those that a mesh axis runs over, the one named last changes fastest.
Arguments:
- state_start: float32 [6, 32, 256, 1024], P(None, 'row', 'gz', 'theta'), may hold values from -1.2 to 1.2
- state_section: float32 [6, 32, 256, 1024], P(None, 'row', 'gz', 'theta'), may hold values from -1.5 to 4, as said below
- phase: int32 [32, 256, 1024], P('row', 'gz', 'theta'), may hold values 0 or 1
- cutoff: int32 [4], replicated, may hold values from 1 to 63
Outputs:
- state_next: float32 [6, 32, 256, 1024], P(None, 'row', 'gz', 'theta')
The draws below stay inside these ranges and needn't reach their ends.
Inputs may be any that keep to these rules, and one draw needn't show every extreme that they name: `state_section`: channel 0 (density) lies in 0.5 to 2.0, channels 1 to 3 (momenta) in -1.5 to 1.5, channel 4 (total energy) in 2.5 to 4.0, channel 5 (jet mass density) in 0 to 1.0.
All inputs are finite; a program needn't handle non-finite values. No bound on the sum of `phase` on one device may be relied on, other than what follows from the above.
Results may differ from the reference program's by a relative error of at most 0.0003.
Values sent between devices are 32-bit elements; how exact they have to be, the bound alone decides.
A program may use at most 64 MiB of HBM per device.

```python
import math
import jax
import jax.numpy as jnp
from jax import lax

NT = 1024
NF = 4
KMODES = 64
NR = 32
NZ = 256


def draw_state_section(key, part):
    subkeys = jax.random.split(jax.random.fold_in(key, 11), 4)
    grid_shape = (NR, NZ, NT)
    density = jax.random.uniform(subkeys[0], grid_shape, minval=0.5, maxval=2.0)
    momenta = jnp.clip(0.3 * jax.random.normal(subkeys[1], (3, NR, NZ, NT)), -1.5, 1.5)
    energy = jax.random.uniform(subkeys[2], grid_shape, minval=2.5, maxval=4.0)
    jet_mass = jax.random.uniform(subkeys[3], grid_shape, minval=0.0, maxval=1.0)
    return jnp.concatenate([density[None], momenta, energy[None], jet_mass[None]], 0).astype(jnp.float32)


def place_ends(values, key, least, largest):
    longest = values.shape.index(max(values.shape))
    spots = []
    for shift in (0, 1):
        where = [jax.random.randint(jax.random.fold_in(key, axis), (), 0, length) for axis, length in enumerate(values.shape)]
        where[longest] = (where[longest] + shift) % values.shape[longest]
        spots.append(tuple(where))
    return values.at[spots[0]].set(least).at[spots[1]].set(largest)


def block_scale(own_key, dims, cuts, low, high):
    def one(position, parts):
        draws = jax.random.uniform(jax.random.fold_in(jax.random.fold_in(own_key, 6), position), (parts,), jnp.float32, low / len(cuts), high / len(cuts))
        return jnp.repeat(jnp.exp(draws), dims[position] // parts).reshape((-1,) + (1,) * (len(dims) - position - 1))

    gain = one(*cuts[0])
    for cut in cuts[1:]:
        gain = gain * one(*cut)
    return gain


def gaussian(rng, dims, scale, most, pieces=(), kind=jnp.bfloat16):
    gain = block_scale(rng, dims, pieces, -0.22, 0.18) if pieces else 1.0
    result = jax.random.normal(rng, dims, jnp.float32) * scale * gain
    return jnp.minimum(jnp.maximum(result, -most), most).astype(kind)


def setup_inputs(seed: int = 0) -> dict:
    splits = jax.random.split(jax.random.key(seed), 5)
    return {
        "state_start": gaussian(splits[0], (6, NR, NZ, NT), 0.2, 1.2, ((1, 8), (2, 8), (3, 4)), jnp.float32),
        "state_section": draw_state_section(jax.random.fold_in(splits[4], 71), 0),
        "phase": place_ends((jax.random.randint(splits[2], (NR, NZ, NT), 0, 3) < 1).astype(jnp.int32), jax.random.fold_in(splits[2], 1), 0, 1),
        "cutoff": place_ends(jax.random.randint(splits[3], (NF,), 1, KMODES), jax.random.fold_in(splits[3], 1), 1, KMODES - 1).astype(jnp.int32),
    }


split_speed = 10.0
time_step = 0.05
weno_epsilon = 1e-6
liquid_ratio = 4.4
gas_ratio = 1.4
liquid_stiffness = 0.6


def pressure_of(state, phase):
    density = state[0]
    kinetic = 0.5 * (state[1] * state[1] + state[2] * state[2] + state[3] * state[3]) / density
    liquid = phase == 1
    heat_ratio = jnp.where(liquid, liquid_ratio, gas_ratio)
    stiffness = jnp.where(liquid, liquid_stiffness, 0.0)
    return (heat_ratio - 1.0) * (state[4] - kinetic) - heat_ratio * stiffness


def weno_face(far_left, near_left, centre, near_right, far_right):
    smooth_left = 13.0 / 12.0 * (far_left - 2.0 * near_left + centre) ** 2 + 0.25 * (far_left - 4.0 * near_left + 3.0 * centre) ** 2
    smooth_mid = 13.0 / 12.0 * (near_left - 2.0 * centre + near_right) ** 2 + 0.25 * (near_left - near_right) ** 2
    smooth_right = 13.0 / 12.0 * (centre - 2.0 * near_right + far_right) ** 2 + 0.25 * (3.0 * centre - 4.0 * near_right + far_right) ** 2
    weight_left = 0.1 / (weno_epsilon + smooth_left) ** 2
    weight_mid = 0.6 / (weno_epsilon + smooth_mid) ** 2
    weight_right = 0.3 / (weno_epsilon + smooth_right) ** 2
    weight_sum = weight_left + weight_mid + weight_right
    value_left = (2.0 * far_left - 7.0 * near_left + 11.0 * centre) / 6.0
    value_mid = (-near_left + 5.0 * centre + 2.0 * near_right) / 6.0
    value_right = (2.0 * centre + 5.0 * near_right - far_right) / 6.0
    return (weight_left * value_left + weight_mid * value_mid + weight_right * value_right) / weight_sum


def face_fluxes(padded_line, array_axis, component):
    density = padded_line[0]
    velocity = padded_line[component] / density
    pressure_field = padded_line[6]
    conserved = padded_line[:6]
    flux_rows = [conserved[channel] * velocity for channel in range(6)]
    flux_rows[component] = flux_rows[component] + pressure_field
    flux_rows[4] = flux_rows[4] + pressure_field * velocity
    physical = jnp.stack(flux_rows)
    upward = 0.5 * (physical + split_speed * conserved)
    downward = 0.5 * (physical - split_speed * conserved)
    face_count = padded_line.shape[array_axis] - 5

    def shifted(values, offset):
        return lax.slice_in_dim(values, offset, offset + face_count, axis=array_axis)

    upwind_part = weno_face(shifted(upward, 0), shifted(upward, 1), shifted(upward, 2), shifted(upward, 3), shifted(upward, 4))
    downwind_part = weno_face(shifted(downward, 5), shifted(downward, 4), shifted(downward, 3), shifted(downward, 2), shifted(downward, 1))
    return upwind_part + downwind_part


def tendency(centre_cells, radial_line, axial_line, azimuth_line, cycle_start):
    cycle_count = centre_cells.shape[1]
    radial_flux = face_fluxes(radial_line, 1, 1)
    axial_flux = face_fluxes(axial_line, 2, 3)
    azimuth_flux = face_fluxes(azimuth_line, 3, 2)
    cycle_index = (cycle_start + lax.iota(jnp.int32, cycle_count + 1)).astype(centre_cells.dtype)
    face_radius = cycle_index[None, :, None, None]
    cell_radius = face_radius[:, :-1] + 0.5
    weighted = face_radius * radial_flux
    div_radial = (weighted[:, 1:] - weighted[:, :-1]) / cell_radius
    div_axial = axial_flux[:, :, 1:] - axial_flux[:, :, :-1]
    angle_step = 2.0 * math.pi / NT
    div_azimuth = (azimuth_flux[..., 1:] - azimuth_flux[..., :-1]) / (cell_radius * angle_step)
    density = centre_cells[0]
    swirl_speed = centre_cells[2] / density
    radius = cell_radius[0]
    source_radial = (centre_cells[2] * swirl_speed + centre_cells[6]) / radius
    source_swirl = -centre_cells[1] * swirl_speed / radius
    zero_field = jnp.zeros_like(density)
    source = jnp.stack([zero_field, source_radial, source_swirl, zero_field, zero_field, zero_field])
    return source - div_radial - div_axial - div_azimuth


def across_axis(partner):
    sign_flip = jnp.array([1.0, -1.0, -1.0, 1.0, 1.0, 1.0, 1.0], partner.dtype)[:, None, None, None]
    return partner[:, ::-1] * sign_flip


def reference(state_start, state_section, phase, cutoff):
    pressure_field = pressure_of(state_section, phase)
    fields = jnp.concatenate([state_section, pressure_field[None]], 0)
    total_depth = fields.shape[2]
    block_size = math.gcd(total_depth, 8)
    block_count = total_depth // block_size

    def one_block(number):
        positions = (number * block_size - 3 + lax.iota(jnp.int32, block_size + 6)) % total_depth
        axial_line = jnp.take(fields, positions.astype(jnp.int32), axis=2)
        centre_cells = axial_line[:, :, 3:-3]
        partner = jnp.roll(centre_cells[:, 0:3], -(NT // 2), axis=3)
        outer_rim = jnp.repeat(centre_cells[:, -1:], 3, axis=1)
        radial_line = jnp.concatenate([across_axis(partner), centre_cells, outer_rim], 1)
        azimuth_line = jnp.concatenate([centre_cells[..., -3:], centre_cells, centre_cells[..., :3]], 3)
        tendencies = tendency(centre_cells, radial_line, axial_line, azimuth_line, 0)
        start_index = (number * block_size).astype(jnp.int32)
        start_block = lax.dynamic_slice_in_dim(state_start, start_index, block_size, 2)
        section_block = lax.dynamic_slice_in_dim(state_section, start_index, block_size, 2)
        return 0.75 * start_block + 0.25 * (section_block + time_step * tendencies)

    block_results = lax.map(one_block, lax.iota(jnp.int32, block_count))
    advanced = jnp.moveaxis(block_results, 0, 2).reshape(state_start.shape)
    inner_block = advanced[:, :NF]
    spectrum = jnp.fft.rfft(inner_block, axis=3)
    mode_index = lax.iota(jnp.int32, NT // 2 + 1)
    kept_modes = mode_index[None, :] <= cutoff[:, None]
    filtered = jnp.fft.irfft(spectrum * kept_modes[None, :, None, :], n=NT, axis=3).astype(advanced.dtype)
    return jnp.concatenate([filtered, advanced[:, NF:]], 1)
```

```python
import functools
import math

import jax
import jax.numpy as jnp
import numpy as np
from jax import lax
from jax.experimental import pallas as pl
from jax.experimental.pallas import tpu as pltpu
from jax.sharding import PartitionSpec as P

NT = 1024
KMODES = 64
GHOST = 3

split_speed = 10.0
time_step = 0.05
weno_epsilon = 1e-06
scaled_epsilon = 4.0 * weno_epsilon * 12.0 / 13.0
side_scale = 3.0 / 13.0

MESH = pl.DeviceIdType.MESH


def primitives(cells, liquid):
    inverse = 1.0 / cells[0]
    kinetic = 0.5 * (cells[1] * cells[1] + cells[2] * cells[2] + cells[3] * cells[3]) * inverse
    internal = cells[4] - kinetic
    pressure = jnp.where(liquid, 3.4 * internal - 4.4 * 0.6, 0.4 * internal)
    return inverse, pressure


def split_flux(cells, velocity, pressure, component, channel):
    flux = cells[channel] * velocity
    if channel == component:
        flux = flux + pressure
    if channel == 4:
        flux = flux + pressure * velocity
    carried = split_speed * cells[channel]
    return flux + carried, flux - carried


def correction(u1, u2, u3, u4, d0, d1, d2, q0, q1, q2):
    a3 = 3.0 * u2
    b3 = 3.0 * u3
    g0 = a3 - u1
    g1 = u2 + u3
    g2 = u4 - b3
    t0 = q0 + (side_scale * g0) * g0
    t1 = q1 + (side_scale * g1) * g1
    t2 = q2 + (side_scale * g2) * g2
    s0 = t0 * t0
    s1 = t1 * t1
    s2 = t2 * t2
    p0 = s1 * s2
    p1 = (6.0 * s0) * s2
    p2 = (3.0 * s0) * s1
    z0 = d0 + d0 + a3
    z1 = g1 + u3
    z2 = b3 - d2
    top = p0 * z0 + p1 * z1 + p2 * z2
    bottom = p0 + p1 + p2
    return (top / bottom) * (1.0 / 6.0)


def line_divergence(upward, downward, axis):
    length = upward.shape[axis]

    def ahead(x, steps):
        return pltpu.roll(x, (-steps) % length, axis)

    def pieces(field):
        u = ahead(field, 1) - field
        um1 = ahead(u, -1)
        um2 = ahead(u, -2)
        up1 = ahead(u, 1)
        d1 = u - um1
        d0 = um1 - um2
        d2 = up1 - u
        return u, um1, um2, up1, d0, d1, d2, d0 * d0 + scaled_epsilon, d1 * d1 + scaled_epsilon, d2 * d2 + scaled_epsilon

    u, um1, um2, up1, d0, d1, d2, q0, q1, q2 = pieces(upward)
    right = upward + correction(um2, um1, u, up1, d0, d1, d2, q0, q1, q2)
    u, um1, um2, up1, d0, d1, d2, q0, q1, q2 = pieces(downward)
    left = downward - correction(up1, u, um1, um2, -d2, -d1, -d0, q2, q1, q0)
    face = right + ahead(left, 1)
    return face - ahead(face, -1)


def kernel(
    start_hbm,
    section_hbm,
    phase_hbm,
    cutoff_smem,
    table_hbm,
    table_t_hbm,
    out_hbm,
    column,
    column_ph,
    result,
    z_low,
    z_low_ph,
    z_high,
    z_high_ph,
    pack_low,
    pack_high,
    got_low,
    got_high,
    table,
    table_t,
    part,
    half_got,
    half_sum,
    half_far,
    half_total,
    half_peer,
    load_sem,
    load_ph_sem,
    rim_sem,
    misc_sem,
    x_send,
    x_recv,
    y_send,
    y_recv,
    m_send,
    z_send,
    z_recv,
    t_send,
    t_recv,
    f_send,
    f_recv,
    out_sem,
):
    row = lax.axis_index("row")
    theta = lax.axis_index("theta")
    gz = lax.axis_index("gz")
    odd = lax.rem(row, 2)
    partner = row + 1 - 2 * odd
    theta_up = lax.rem(theta + 1, 4)
    theta_down = lax.rem(theta + 3, 4)
    theta_far = lax.rem(theta + 2, 4)
    sibling = theta + 1 - 2 * lax.rem(theta, 2)
    gz_up = lax.rem(gz + 1, 8)
    gz_down = lax.rem(gz + 7, 8)
    first = row == 0
    last = row == 7

    def piece(k):
        octet = k // 2
        half = k % 2
        if isinstance(k, int):
            return pl.ds(octet * 8, 8), pl.ds(half * 128, 128)
        return pl.ds(pl.multiple_of(octet * 8, 8), 8), pl.ds(pl.multiple_of(half * 128, 128), 128)

    def load(k):
        rows, lanes = piece(k)
        return (
            pltpu.make_async_copy(section_hbm.at[:, :, rows, lanes], column.at[:, pl.ds(4, 4), rows, lanes], load_sem.at[k]),
            pltpu.make_async_copy(phase_hbm.at[:, rows, lanes], column_ph.at[pl.ds(4, 4), rows, lanes], load_ph_sem.at[k]),
        )

    for k in range(8):
        for copy in load(k):
            copy.start()
    start_copy = pltpu.make_async_copy(start_hbm, result, misc_sem.at[0])
    start_copy.start()

    def rims():
        copies = []
        for j in range(3):
            copies.append(pltpu.make_async_copy(section_hbm.at[:, pl.ds(3, 1)], column.at[:, pl.ds(8 + j, 1)], rim_sem.at[2 * j]))
            copies.append(pltpu.make_async_copy(phase_hbm.at[pl.ds(3, 1)], column_ph.at[pl.ds(8 + j, 1)], rim_sem.at[2 * j + 1]))
        return copies

    def table_loads():
        return (
            pltpu.make_async_copy(table_hbm.at[pl.ds(pl.multiple_of(theta * 256, 256), 256)], table, misc_sem.at[1]),
            pltpu.make_async_copy(table_t_hbm.at[theta], table_t, misc_sem.at[2]),
        )

    @pl.when(last)
    def _():
        for copy in rims():
            copy.start()

    @pl.when(first)
    def _():
        for copy in table_loads():
            copy.start()

    barrier = pltpu.get_barrier_semaphore()
    for where in (
        {"row": partner},
        {"row": lax.rem(row + 2, 8)},
        {"row": lax.rem(row + 6, 8)},
        {"theta": theta_up},
        {"theta": theta_down},
        {"theta": theta_far},
        {"gz": gz_up},
        {"gz": gz_down},
    ):
        pl.semaphore_signal(barrier, inc=1, device_id=where, device_id_type=MESH)
    pl.semaphore_wait(barrier, 8)

    def carry(k, source, target, count, send, recv, where):
        rows, lanes = piece(k)
        return (
            pltpu.make_async_remote_copy(
                src_ref=column.at[:, pl.ds(source, count), rows, lanes],
                dst_ref=column.at[:, pl.ds(target, count), rows, lanes],
                send_sem=send.at[k],
                recv_sem=recv.at[k],
                device_id=where,
                device_id_type=MESH,
            ),
            pltpu.make_async_remote_copy(
                src_ref=column_ph.at[pl.ds(source, count), rows, lanes],
                dst_ref=column_ph.at[pl.ds(target, count), rows, lanes],
                send_sem=send.at[k + 8],
                recv_sem=recv.at[k + 8],
                device_id=where,
                device_id_type=MESH,
            ),
        )

    inner_row = jnp.logical_and(row > 0, row < 7)
    to_partner = {"row": partner}

    def x_full(k):
        return carry(k, 4, 8 * odd, 4, x_send, x_recv, to_partner)

    def x_first(k):
        return carry(k, 5, 1, 3, x_send, x_recv, to_partner)

    def x_last(k):
        return carry(k, 4, 8, 3, x_send, x_recv, to_partner)

    def mirror(k):
        return carry(k, 4, 1, 3, m_send, y_recv, {"theta": theta_far})

    def forward(k):
        target = jnp.where(odd == 1, lax.rem(row + 6, 8), lax.rem(row + 2, 8))
        return carry(k, 9 - 9 * odd, 1 + 7 * odd, 3, y_send, y_recv, {"row": target})

    forwards = jnp.logical_or(jnp.logical_and(odd == 0, row < 6), jnp.logical_and(odd == 1, row > 1))

    def z_copies():
        copies = []
        for side, (rows, cells_to, phase_to, where) in enumerate(
            (
                (pl.ds(0, 8), z_high, z_high_ph, {"gz": gz_down}),
                (pl.ds(24, 8), z_low, z_low_ph, {"gz": gz_up}),
            )
        ):
            copies.append(
                pltpu.make_async_remote_copy(
                    src_ref=column.at[:, pl.ds(4, 4), rows, :],
                    dst_ref=cells_to,
                    send_sem=z_send.at[2 * side],
                    recv_sem=z_recv.at[2 * side],
                    device_id=where,
                    device_id_type=MESH,
                )
            )
            copies.append(
                pltpu.make_async_remote_copy(
                    src_ref=column_ph.at[pl.ds(4, 4), rows, :],
                    dst_ref=phase_to,
                    send_sem=z_send.at[2 * side + 1],
                    recv_sem=z_recv.at[2 * side + 1],
                    device_id=where,
                    device_id_type=MESH,
                )
            )
        return copies

    for k in range(8):
        for copy in load(k):
            copy.wait()

        @pl.when(inner_row)
        def _():
            for copy in x_full(k):
                copy.start()

        @pl.when(first)
        def _():
            for copy in x_first(k):
                copy.start()
            for copy in mirror(k):
                copy.start()

        @pl.when(last)
        def _():
            for copy in x_last(k):
                copy.start()

    for copy in z_copies():
        copy.start()

    lane = lax.broadcasted_iota(jnp.int32, (8, 128), 1)

    def pack(n, _):
        pair = n // 4
        rows = pl.ds(pl.multiple_of((n % 4) * 8, 8), 8)
        low = jnp.zeros((8, 128), jnp.float32)
        high = jnp.zeros((8, 128), jnp.float32)
        for group in range(14):
            channel, cycle = group % 7, 4 + 2 * pair + group // 7
            if channel < 6:
                near = column[channel, cycle, rows, pl.ds(0, 128)]
                far = column[channel, cycle, rows, pl.ds(128, 128)]
            else:
                near = column_ph[cycle, rows, pl.ds(0, 128)].astype(jnp.float32)
                far = column_ph[cycle, rows, pl.ds(128, 128)].astype(jnp.float32)
            if group:
                near = pltpu.roll(near, 8 * group, 1)
            far = pltpu.roll(far, (8 * group + 8) % 128, 1)
            here = lane // 8 == group
            low = jnp.where(here, near, low)
            high = jnp.where(here, far, high)
        pack_low[pair, rows, :] = low
        pack_high[pair, rows, :] = high
        return 0

    lax.fori_loop(0, 8, pack, 0)

    def t_copies():
        return (
            pltpu.make_async_remote_copy(
                src_ref=pack_low,
                dst_ref=got_high,
                send_sem=t_send.at[0],
                recv_sem=t_recv.at[0],
                device_id={"theta": theta_down},
                device_id_type=MESH,
            ),
            pltpu.make_async_remote_copy(
                src_ref=pack_high,
                dst_ref=got_low,
                send_sem=t_send.at[1],
                recv_sem=t_recv.at[1],
                device_id={"theta": theta_up},
                device_id_type=MESH,
            ),
        )

    for copy in t_copies():
        copy.start()
    start_copy.wait()
    for copy in t_copies():
        copy.wait_recv()

    quarter = 0.25 * time_step

    def azimuthal(n, _):
        cycle = n // 4
        octet = n % 4
        rows = pl.ds(pl.multiple_of(octet * 8, 8), 8)
        pair = cycle // 2
        low = got_low[pair, rows, :]
        high = got_high[pair, rows, :]
        base = lax.rem(cycle, 2) * 56

        def edge(channel):
            offset = base + 8 * channel
            upper = pltpu.roll(high, lax.rem(128 - offset, 128), 1)
            lower = pltpu.roll(low, 120 - offset, 1)
            return jnp.where(lane < 64, upper, lower)

        cells = [jnp.concatenate([column[c, 4 + cycle, rows, :], edge(c)], 1) for c in range(6)]
        material = jnp.concatenate([column_ph[4 + cycle, rows, :].astype(jnp.float32), edge(6)], 1)
        inverse, pressure = primitives(cells, material > 0.5)
        velocity = cells[2] * inverse
        radius = (row * 4 + cycle).astype(jnp.float32) + 0.5
        scale = 0.5 * quarter / (radius * (2.0 * math.pi / NT))
        source_scale = quarter / radius
        for c in range(6):
            upward, downward = split_flux(cells, velocity, pressure, 2, c)
            change = line_divergence(upward, downward, 1)[:, :256] * scale
            value = 0.75 * result[c, cycle, rows, :] + 0.25 * cells[c][:, :256] - change
            if c == 1:
                value = value + source_scale * (cells[2] * velocity + pressure)[:, :256]
            if c == 2:
                value = value - source_scale * (cells[1] * velocity)[:, :256]
            result[c, cycle, rows, :] = value
        return 0

    lax.fori_loop(0, 16, azimuthal, 0)

    row8 = lax.broadcasted_iota(jnp.int32, (8, 128), 0)

    def axial(n):
        cycle = n // 2
        lanes = pl.ds(pl.multiple_of((n % 2) * 128, 128), 128)
        cells = [
            jnp.concatenate(
                [column[c, 4 + cycle, :, lanes], jnp.where(row8 < 4, z_high[c, cycle, :, lanes], z_low[c, cycle, :, lanes])], 0
            )
            for c in range(6)
        ]
        material = jnp.concatenate(
            [column_ph[4 + cycle, :, lanes], jnp.where(row8 < 4, z_high_ph[cycle, :, lanes], z_low_ph[cycle, :, lanes])], 0
        )
        inverse, pressure = primitives(cells, material == 1)
        velocity = cells[3] * inverse
        for c in range(6):
            upward, downward = split_flux(cells, velocity, pressure, 3, c)
            change = line_divergence(upward, downward, 0)[:32] * (0.5 * quarter)
            result[c, cycle, :, lanes] = result[c, cycle, :, lanes] - change

    def arrive_and_forward(k):
        @pl.when(jnp.logical_and(row != 1, row != 6))
        def _():
            for copy in carry(k, 4, 4, 4, x_send, x_recv, to_partner):
                copy.wait_recv()

        @pl.when(jnp.logical_or(row == 1, row == 6))
        def _():
            for copy in carry(k, 4, 4, 3, x_send, x_recv, to_partner):
                copy.wait_recv()

        @pl.when(forwards)
        def _():
            for copy in forward(k):
                copy.start()

    def y_arrive(k):
        @pl.when(row != 7)
        def _():
            for copy in carry(k, 4, 4, 3, y_send, y_recv, to_partner):
                copy.wait_recv()

    flip = jnp.where(first, -1.0, 1.0)

    def radial(k):
        rows, lanes = piece(k)
        planes = [jnp.where(first, 4 - p, p) for p in (1, 2, 3)] + list(range(4, 11))
        stack = []
        for i, plane in enumerate(planes):
            cells = [column[c, plane, rows, lanes] for c in range(6)]
            if i < 3:
                cells[1] = cells[1] * flip
                cells[2] = cells[2] * flip
            inverse, pressure = primitives(cells, column_ph[plane, rows, lanes] == 1)
            stack.append((cells, cells[1] * inverse, pressure))
        for c in range(6):
            up, down = zip(*[split_flux(cells, v, p, 1, c) for cells, v, p in stack])

            def pieces(field):
                u = [field[i + 1] - field[i] for i in range(9)]
                d = [None] + [u[i] - u[i - 1] for i in range(1, 9)]
                q = [None] + [d[i] * d[i] + scaled_epsilon for i in range(1, 9)]
                return u, d, q

            u, d, q = pieces(up)
            right = [
                up[i] + correction(u[i - 2], u[i - 1], u[i], u[i + 1], d[i - 1], d[i], d[i + 1], q[i - 1], q[i], q[i + 1])
                for i in range(2, 7)
            ]
            u, d, q = pieces(down)
            left = [
                down[i] - correction(u[i + 1], u[i], u[i - 1], u[i - 2], -d[i + 1], -d[i], -d[i - 1], q[i + 1], q[i], q[i - 1])
                for i in range(3, 8)
            ]
            face = [a + b for a, b in zip(right, left)]
            weighted = [(row * 4 + j).astype(jnp.float32) * face[j] for j in range(5)]
            for j in range(4):
                radius = (row * 4 + j).astype(jnp.float32) + 0.5
                result[c, j, rows, lanes] = result[c, j, rows, lanes] - (weighted[j + 1] - weighted[j]) * (0.5 * quarter / radius)

    for copy in z_copies():
        copy.wait_recv()
    arrive_and_forward(0)

    def axial_pair(n, _):
        axial(2 * n)
        axial(2 * n + 1)
        arrive_and_forward(n + 1)
        return 0

    lax.fori_loop(0, 4, axial_pair, 0)

    @pl.when(last)
    def _():
        for copy in rims():
            copy.wait()

    def radial_step(k, _):
        @pl.when(k + 5 < 8)
        def _():
            arrive_and_forward(k + 5)

        y_arrive(k)
        radial(k)
        return 0

    lax.fori_loop(0, 8, radial_step, 0)

    def out_copy(o):
        rows = pl.ds(o * 8, 8)
        return pltpu.make_async_copy(result.at[:, :, rows, :], out_hbm.at[:, :, rows, :], out_sem.at[o])

    @pl.when(first)
    def _():
        for copy in table_loads():
            copy.wait()
        mine = lax.rem(theta, 2) * 96
        other = 96 - mine
        pairs = ((0, {"theta": sibling}), (4, {"theta": theta_far}), (8, {"theta": sibling}))

        def share(step, o, source, target):
            base, where = pairs[step]
            return pltpu.make_async_remote_copy(
                src_ref=source,
                dst_ref=target,
                send_sem=f_send.at[base + o],
                recv_sem=f_recv.at[base + o],
                device_id=where,
                device_id_type=MESH,
            )

        def step_one(o):
            return share(0, o, part.at[o, pl.ds(pl.multiple_of(other, 8), 96)], half_got.at[o])

        def step_two(o):
            return share(1, o, half_sum.at[o], half_far.at[o])

        def step_three(o):
            return share(2, o, half_total.at[o], half_peer.at[o])

        for o in range(4):
            values = result[:, :, pl.ds(8 * o, 8), :].reshape(192, 256)
            part[o] = jnp.dot(values, table[...], precision=lax.Precision.HIGHEST, preferred_element_type=jnp.float32)
            step_one(o).start()
        for o in range(4):
            step_one(o).wait_recv()
            half_sum[o] = part[o, pl.ds(pl.multiple_of(mine, 8), 96)] + half_got[o]
            step_two(o).start()
        for o in range(4):
            step_two(o).wait_recv()
            half_total[o] = half_sum[o] + half_far[o]
            step_three(o).start()
        order = lax.broadcasted_iota(jnp.int32, (8, 128), 1)
        order = jnp.where(order < KMODES, order, order - KMODES)
        mode_scale = jnp.where(order == 0, 1.0 / NT, 2.0 / NT)
        weights = [jnp.where(order <= cutoff_smem[i], mode_scale, 0.0) for i in range(4)]
        weights = jnp.concatenate(weights * 3, 0)
        even_core = mine == 0
        for o in range(4):
            step_three(o).wait_recv()
            own = half_total[o] * weights
            peer = half_peer[o] * weights
            lower = jnp.where(even_core, own, peer)
            upper = jnp.where(even_core, peer, own)
            coefficients = jnp.concatenate([lower, upper], 0)
            values = jnp.dot(coefficients, table_t[...], precision=lax.Precision.HIGHEST, preferred_element_type=jnp.float32)
            result[:, :, pl.ds(8 * o, 8), :] = values.reshape(6, 4, 8, 256)
            out_copy(o).start()
        for o in range(4):
            step_one(o).wait_send()
            step_two(o).wait_send()
            step_three(o).wait_send()

    @pl.when(jnp.logical_not(first))
    def _():
        for o in range(4):
            out_copy(o).start()

    for copy in t_copies():
        copy.wait_send()
    for copy in z_copies():
        copy.wait_send()
    for k in range(8):

        @pl.when(inner_row)
        def _():
            for copy in x_full(k):
                copy.wait_send()

        @pl.when(jnp.logical_not(inner_row))
        def _():
            for copy in x_last(k):
                copy.wait_send()

        @pl.when(first)
        def _():
            for copy in mirror(k):
                copy.wait_send()

        @pl.when(forwards)
        def _():
            for copy in forward(k):
                copy.wait_send()

    for o in range(4):
        out_copy(o).wait()


def fourier_tables():
    phases = (np.arange(NT)[:, None] * np.arange(KMODES)[None, :]) % NT
    angles = phases.astype(np.float64) * (2.0 * np.pi / NT)
    table = np.concatenate([np.cos(angles), np.sin(angles)], 1).astype(np.float32)
    return table, np.ascontiguousarray(table.reshape(4, 256, 2 * KMODES).transpose(0, 2, 1))


def shards(state_start, state_section, phase, cutoff):
    f32, i32 = jnp.float32, jnp.int32
    table, table_t = fourier_tables()
    anywhere = pl.BlockSpec(memory_space=pl.ANY)
    dma = pltpu.SemaphoreType.DMA
    return pl.pallas_call(
        kernel,
        out_shape=jax.ShapeDtypeStruct(state_start.shape, f32),
        in_specs=[anywhere, anywhere, anywhere, pl.BlockSpec(memory_space=pltpu.SMEM), anywhere, anywhere],
        out_specs=anywhere,
        scratch_shapes=[
            pltpu.VMEM((6, 12, 32, 256), f32),
            pltpu.VMEM((12, 32, 256), i32),
            pltpu.VMEM((6, 4, 32, 256), f32),
            pltpu.VMEM((6, 4, 8, 256), f32),
            pltpu.VMEM((4, 8, 256), i32),
            pltpu.VMEM((6, 4, 8, 256), f32),
            pltpu.VMEM((4, 8, 256), i32),
            pltpu.VMEM((2, 32, 128), f32),
            pltpu.VMEM((2, 32, 128), f32),
            pltpu.VMEM((2, 32, 128), f32),
            pltpu.VMEM((2, 32, 128), f32),
            pltpu.VMEM((256, 2 * KMODES), f32),
            pltpu.VMEM((2 * KMODES, 256), f32),
            pltpu.VMEM((4, 192, 2 * KMODES), f32),
            pltpu.VMEM((4, 96, 2 * KMODES), f32),
            pltpu.VMEM((4, 96, 2 * KMODES), f32),
            pltpu.VMEM((4, 96, 2 * KMODES), f32),
            pltpu.VMEM((4, 96, 2 * KMODES), f32),
            pltpu.VMEM((4, 96, 2 * KMODES), f32),
            dma((8,)),
            dma((8,)),
            dma((6,)),
            dma((3,)),
            dma((16,)),
            dma((16,)),
            dma((16,)),
            dma((16,)),
            dma((16,)),
            dma((4,)),
            dma((4,)),
            dma((2,)),
            dma((2,)),
            dma((12,)),
            dma((12,)),
            dma((4,)),
        ],
        compiler_params=pltpu.CompilerParams(collective_id=0, has_side_effects=True, vmem_limit_bytes=40 * 1024 * 1024),
        name="jet_section",
    )(state_start, state_section, phase, cutoff, jnp.asarray(table), jnp.asarray(table_t))


def solution(mesh):
    in_specs = (
        P(None, "row", "gz", "theta"),
        P(None, "row", "gz", "theta"),
        P("row", "gz", "theta"),
        P(),
    )
    out_specs = P(None, "row", "gz", "theta")
    return jax.shard_map(shards, mesh=mesh, in_specs=in_specs, out_specs=out_specs, check_vma=False)
```

```python
import functools
import math

import jax
import jax.numpy as jnp
import numpy as np
from jax import lax
from jax.experimental import pallas as pl
from jax.experimental.pallas import tpu as pltpu
from jax.sharding import PartitionSpec as P

NT = 1024
KMODES = 64
GHOST = 3

split_speed = 10.0
time_step = 0.05
weno_epsilon = 1e-06
scaled_epsilon = 4.0 * weno_epsilon * 12.0 / 13.0
side_scale = 3.0 / 13.0

MESH = pl.DeviceIdType.MESH


def primitives(cells, liquid):
    inverse = 1.0 / cells[0]
    kinetic = 0.5 * (cells[1] * cells[1] + cells[2] * cells[2] + cells[3] * cells[3]) * inverse
    internal = cells[4] - kinetic
    pressure = jnp.where(liquid, 3.4 * internal - 4.4 * 0.6, 0.4 * internal)
    return inverse, pressure


def split_flux(cells, velocity, pressure, component, channel):
    flux = cells[channel] * velocity
    if channel == component:
        flux = flux + pressure
    if channel == 4:
        flux = flux + pressure * velocity
    carried = split_speed * cells[channel]
    return flux + carried, flux - carried


def correction(u1, u2, u3, u4, d0, d1, d2, q0, q1, q2):
    a3 = 3.0 * u2
    b3 = 3.0 * u3
    g0 = a3 - u1
    g1 = u2 + u3
    g2 = u4 - b3
    t0 = q0 + (side_scale * g0) * g0
    t1 = q1 + (side_scale * g1) * g1
    t2 = q2 + (side_scale * g2) * g2
    s0 = t0 * t0
    s1 = t1 * t1
    s2 = t2 * t2
    p0 = s1 * s2
    p1 = (6.0 * s0) * s2
    p2 = (3.0 * s0) * s1
    z0 = d0 + d0 + a3
    z1 = g1 + u3
    z2 = b3 - d2
    top = p0 * z0 + p1 * z1 + p2 * z2
    bottom = p0 + p1 + p2
    return (top / bottom) * (1.0 / 6.0)


def line_divergence(upward, downward, axis):
    length = upward.shape[axis]

    def ahead(x, steps):
        return pltpu.roll(x, (-steps) % length, axis)

    def pieces(field):
        u = ahead(field, 1) - field
        um1 = ahead(u, -1)
        um2 = ahead(u, -2)
        up1 = ahead(u, 1)
        d1 = u - um1
        d0 = um1 - um2
        d2 = up1 - u
        return u, um1, um2, up1, d0, d1, d2, d0 * d0 + scaled_epsilon, d1 * d1 + scaled_epsilon, d2 * d2 + scaled_epsilon

    u, um1, um2, up1, d0, d1, d2, q0, q1, q2 = pieces(upward)
    right = upward + correction(um2, um1, u, up1, d0, d1, d2, q0, q1, q2)
    u, um1, um2, up1, d0, d1, d2, q0, q1, q2 = pieces(downward)
    left = downward - correction(up1, u, um1, um2, -d2, -d1, -d0, q2, q1, q0)
    face = right + ahead(left, 1)
    return face - ahead(face, -1)


def kernel(
    start_hbm,
    section_hbm,
    phase_hbm,
    cutoff_hbm,
    table_hbm,
    table_t_hbm,
    out_hbm,
    column,
    column_ph,
    result,
    z_low,
    z_low_ph,
    z_high,
    z_high_ph,
    pack_low,
    pack_high,
    got_low,
    got_high,
    table,
    table_t,
    part,
    half_got,
    half_sum,
    half_far,
    half_total,
    half_peer,
    cutoff_smem,
    load_sem,
    load_ph_sem,
    rim_sem,
    misc_sem,
    x_send,
    x_recv,
    y_send,
    y_recv,
    m_send,
    z_send,
    z_recv,
    t_send,
    t_recv,
    f_send,
    f_recv,
    out_sem,
):
    row = lax.axis_index("row")
    theta = lax.axis_index("theta")
    gz = lax.axis_index("gz")
    odd = lax.rem(row, 2)
    partner = row + 1 - 2 * odd
    theta_up = lax.rem(theta + 1, 4)
    theta_down = lax.rem(theta + 3, 4)
    theta_far = lax.rem(theta + 2, 4)
    sibling = theta + 1 - 2 * lax.rem(theta, 2)
    gz_up = lax.rem(gz + 1, 8)
    gz_down = lax.rem(gz + 7, 8)
    first = row == 0
    last = row == 7

    def piece(k):
        octet = k // 2
        half = k % 2
        if isinstance(k, int):
            return pl.ds(octet * 8, 8), pl.ds(half * 128, 128)
        return pl.ds(pl.multiple_of(octet * 8, 8), 8), pl.ds(pl.multiple_of(half * 128, 128), 128)

    def load(k):
        rows, lanes = piece(k)
        return (
            pltpu.make_async_copy(section_hbm.at[:, :, rows, lanes], column.at[:, pl.ds(4, 4), rows, lanes], load_sem.at[k]),
            pltpu.make_async_copy(phase_hbm.at[:, rows, lanes], column_ph.at[pl.ds(4, 4), rows, lanes], load_ph_sem.at[k]),
        )

    for k in range(8):
        for copy in load(k):
            copy.start()
    start_copy = pltpu.make_async_copy(start_hbm, result, misc_sem.at[0])
    start_copy.start()

    def rims():
        copies = []
        for j in range(3):
            copies.append(pltpu.make_async_copy(section_hbm.at[:, pl.ds(3, 1)], column.at[:, pl.ds(8 + j, 1)], rim_sem.at[2 * j]))
            copies.append(pltpu.make_async_copy(phase_hbm.at[pl.ds(3, 1)], column_ph.at[pl.ds(8 + j, 1)], rim_sem.at[2 * j + 1]))
        return copies

    def table_loads():
        return (
            pltpu.make_async_copy(table_hbm.at[pl.ds(pl.multiple_of(theta * 256, 256), 256)], table, misc_sem.at[1]),
            pltpu.make_async_copy(table_t_hbm.at[theta], table_t, misc_sem.at[2]),
            pltpu.make_async_copy(cutoff_hbm, cutoff_smem, misc_sem.at[3]),
        )

    @pl.when(last)
    def _():
        for copy in rims():
            copy.start()

    @pl.when(first)
    def _():
        for copy in table_loads():
            copy.start()

    barrier = pltpu.get_barrier_semaphore()
    for where in (
        {"row": partner},
        {"row": lax.rem(row + 2, 8)},
        {"row": lax.rem(row + 6, 8)},
        {"theta": theta_up},
        {"theta": theta_down},
        {"theta": theta_far},
        {"gz": gz_up},
        {"gz": gz_down},
    ):
        pl.semaphore_signal(barrier, inc=1, device_id=where, device_id_type=MESH)

    def carry(k, source, target, count, send, recv, where):
        rows, lanes = piece(k)
        return (
            pltpu.make_async_remote_copy(
                src_ref=column.at[:, pl.ds(source, count), rows, lanes],
                dst_ref=column.at[:, pl.ds(target, count), rows, lanes],
                send_sem=send.at[k],
                recv_sem=recv.at[k],
                device_id=where,
                device_id_type=MESH,
            ),
            pltpu.make_async_remote_copy(
                src_ref=column_ph.at[pl.ds(source, count), rows, lanes],
                dst_ref=column_ph.at[pl.ds(target, count), rows, lanes],
                send_sem=send.at[k + 8],
                recv_sem=recv.at[k + 8],
                device_id=where,
                device_id_type=MESH,
            ),
        )

    for k in range(8):
        for copy in load(k):
            copy.wait()

    lane = lax.broadcasted_iota(jnp.int32, (8, 128), 1)

    def pack(n, _):
        pair = n // 4
        rows = pl.ds(pl.multiple_of((n % 4) * 8, 8), 8)
        low = jnp.zeros((8, 128), jnp.float32)
        high = jnp.zeros((8, 128), jnp.float32)
        for group in range(14):
            channel, cycle = group % 7, 4 + 2 * pair + group // 7
            if channel < 6:
                near = column[channel, cycle, rows, pl.ds(0, 128)]
                far = column[channel, cycle, rows, pl.ds(128, 128)]
            else:
                near = column_ph[cycle, rows, pl.ds(0, 128)].astype(jnp.float32)
                far = column_ph[cycle, rows, pl.ds(128, 128)].astype(jnp.float32)
            if group:
                near = pltpu.roll(near, 8 * group, 1)
            far = pltpu.roll(far, (8 * group + 8) % 128, 1)
            here = lane // 8 == group
            low = jnp.where(here, near, low)
            high = jnp.where(here, far, high)
        pack_low[pair, rows, :] = low
        pack_high[pair, rows, :] = high
        return 0

    lax.fori_loop(0, 8, pack, 0)

    inner_row = jnp.logical_and(row > 0, row < 7)
    to_partner = {"row": partner}

    def x_full(k):
        return carry(k, 4, 8 * odd, 4, x_send, x_recv, to_partner)

    def x_first(k):
        return carry(k, 5, 1, 3, x_send, x_recv, to_partner)

    def x_last(k):
        return carry(k, 4, 8, 3, x_send, x_recv, to_partner)

    def mirror(k):
        return carry(k, 4, 1, 3, m_send, y_recv, {"theta": theta_far})

    def forward(k):
        target = jnp.where(odd == 1, lax.rem(row + 6, 8), lax.rem(row + 2, 8))
        return carry(k, 9 - 9 * odd, 1 + 7 * odd, 3, y_send, y_recv, {"row": target})

    forwards = jnp.logical_or(jnp.logical_and(odd == 0, row < 6), jnp.logical_and(odd == 1, row > 1))

    def z_copies():
        copies = []
        for side, (rows, cells_to, phase_to, where) in enumerate(
            (
                (pl.ds(0, 8), z_high, z_high_ph, {"gz": gz_down}),
                (pl.ds(24, 8), z_low, z_low_ph, {"gz": gz_up}),
            )
        ):
            copies.append(
                pltpu.make_async_remote_copy(
                    src_ref=column.at[:, pl.ds(4, 4), rows, :],
                    dst_ref=cells_to,
                    send_sem=z_send.at[2 * side],
                    recv_sem=z_recv.at[2 * side],
                    device_id=where,
                    device_id_type=MESH,
                )
            )
            copies.append(
                pltpu.make_async_remote_copy(
                    src_ref=column_ph.at[pl.ds(4, 4), rows, :],
                    dst_ref=phase_to,
                    send_sem=z_send.at[2 * side + 1],
                    recv_sem=z_recv.at[2 * side + 1],
                    device_id=where,
                    device_id_type=MESH,
                )
            )
        return copies

    def t_copies():
        return (
            pltpu.make_async_remote_copy(
                src_ref=pack_low,
                dst_ref=got_high,
                send_sem=t_send.at[0],
                recv_sem=t_recv.at[0],
                device_id={"theta": theta_down},
                device_id_type=MESH,
            ),
            pltpu.make_async_remote_copy(
                src_ref=pack_high,
                dst_ref=got_low,
                send_sem=t_send.at[1],
                recv_sem=t_recv.at[1],
                device_id={"theta": theta_up},
                device_id_type=MESH,
            ),
        )

    pl.semaphore_wait(barrier, 8)
    for copy in t_copies():
        copy.start()
    for copy in z_copies():
        copy.start()

    for k in range(8):

        @pl.when(inner_row)
        def _():
            for copy in x_full(k):
                copy.start()

        @pl.when(first)
        def _():
            for copy in x_first(k):
                copy.start()
            for copy in mirror(k):
                copy.start()

        @pl.when(last)
        def _():
            for copy in x_last(k):
                copy.start()

    start_copy.wait()
    for copy in t_copies():
        copy.wait_recv()

    quarter = 0.25 * time_step

    def azimuthal(n, _):
        cycle = n // 4
        octet = n % 4
        rows = pl.ds(pl.multiple_of(octet * 8, 8), 8)
        pair = cycle // 2
        low = got_low[pair, rows, :]
        high = got_high[pair, rows, :]
        base = lax.rem(cycle, 2) * 56

        def edge(channel):
            offset = base + 8 * channel
            upper = pltpu.roll(high, lax.rem(128 - offset, 128), 1)
            lower = pltpu.roll(low, 120 - offset, 1)
            return jnp.where(lane < 64, upper, lower)

        cells = [jnp.concatenate([column[c, 4 + cycle, rows, :], edge(c)], 1) for c in range(6)]
        old = [result[c, cycle, rows, :] for c in range(6)]
        new = []
        material = jnp.concatenate([column_ph[4 + cycle, rows, :].astype(jnp.float32), edge(6)], 1)
        inverse, pressure = primitives(cells, material > 0.5)
        velocity = cells[2] * inverse
        radius = (row * 4 + cycle).astype(jnp.float32) + 0.5
        scale = 0.5 * quarter / (radius * (2.0 * math.pi / NT))
        source_scale = quarter / radius
        for c in range(6):
            upward, downward = split_flux(cells, velocity, pressure, 2, c)
            change = line_divergence(upward, downward, 1)[:, :256] * scale
            value = 0.75 * old[c] + 0.25 * cells[c][:, :256] - change
            if c == 1:
                value = value + source_scale * (cells[2] * velocity + pressure)[:, :256]
            if c == 2:
                value = value - source_scale * (cells[1] * velocity)[:, :256]
            new.append(value)
        for c in range(6):
            result[c, cycle, rows, :] = new[c]
        return 0

    row8 = lax.broadcasted_iota(jnp.int32, (8, 128), 0)

    def axial(n):
        cycle = n // 2
        lanes = pl.ds(pl.multiple_of((n % 2) * 128, 128), 128)
        cells = [
            jnp.concatenate(
                [column[c, 4 + cycle, :, lanes], jnp.where(row8 < 4, z_high[c, cycle, :, lanes], z_low[c, cycle, :, lanes])], 0
            )
            for c in range(6)
        ]
        material = jnp.concatenate(
            [column_ph[4 + cycle, :, lanes], jnp.where(row8 < 4, z_high_ph[cycle, :, lanes], z_low_ph[cycle, :, lanes])], 0
        )
        inverse, pressure = primitives(cells, material == 1)
        velocity = cells[3] * inverse
        for c in range(6):
            upward, downward = split_flux(cells, velocity, pressure, 3, c)
            change = line_divergence(upward, downward, 0)[:32] * (0.5 * quarter)
            result[c, cycle, :, lanes] = result[c, cycle, :, lanes] - change

    def arrive_and_forward(k):
        @pl.when(jnp.logical_and(row != 1, row != 6))
        def _():
            for copy in carry(k, 4, 4, 4, x_send, x_recv, to_partner):
                copy.wait_recv()

        @pl.when(jnp.logical_or(row == 1, row == 6))
        def _():
            for copy in carry(k, 4, 4, 3, x_send, x_recv, to_partner):
                copy.wait_recv()

        @pl.when(forwards)
        def _():
            for copy in forward(k):
                copy.start()

    def y_arrive(k):
        @pl.when(row != 7)
        def _():
            for copy in carry(k, 4, 4, 3, y_send, y_recv, to_partner):
                copy.wait_recv()

    flip = jnp.where(first, -1.0, 1.0)

    def radial(k):
        rows, lanes = piece(k)
        planes = [jnp.where(first, 4 - p, p) for p in (1, 2, 3)] + list(range(4, 11))
        stack = []
        for i, plane in enumerate(planes):
            cells = [column[c, plane, rows, lanes] for c in range(6)]
            if i < 3:
                cells[1] = cells[1] * flip
                cells[2] = cells[2] * flip
            inverse, pressure = primitives(cells, column_ph[plane, rows, lanes] == 1)
            stack.append((cells, cells[1] * inverse, pressure))
        for c in range(6):
            up, down = zip(*[split_flux(cells, v, p, 1, c) for cells, v, p in stack])

            def pieces(field):
                u = [field[i + 1] - field[i] for i in range(9)]
                d = [None] + [u[i] - u[i - 1] for i in range(1, 9)]
                q = [None] + [d[i] * d[i] + scaled_epsilon for i in range(1, 9)]
                return u, d, q

            u, d, q = pieces(up)
            right = [
                up[i] + correction(u[i - 2], u[i - 1], u[i], u[i + 1], d[i - 1], d[i], d[i + 1], q[i - 1], q[i], q[i + 1])
                for i in range(2, 7)
            ]
            u, d, q = pieces(down)
            left = [
                down[i] - correction(u[i + 1], u[i], u[i - 1], u[i - 2], -d[i + 1], -d[i], -d[i - 1], q[i + 1], q[i], q[i - 1])
                for i in range(3, 8)
            ]
            face = [a + b for a, b in zip(right, left)]
            weighted = [(row * 4 + j).astype(jnp.float32) * face[j] for j in range(5)]
            for j in range(4):
                radius = (row * 4 + j).astype(jnp.float32) + 0.5
                result[c, j, rows, lanes] = result[c, j, rows, lanes] - (weighted[j + 1] - weighted[j]) * (0.5 * quarter / radius)

    def axial_step(n, _):
        axial(n)
        return 0

    lax.fori_loop(0, 8, azimuthal, 0)
    arrive_and_forward(0)
    lax.fori_loop(8, 12, azimuthal, 0)
    arrive_and_forward(1)
    lax.fori_loop(12, 16, azimuthal, 0)
    arrive_and_forward(2)
    for copy in z_copies():
        copy.wait_recv()
    lax.fori_loop(0, 4, axial_step, 0)
    arrive_and_forward(3)
    lax.fori_loop(4, 8, axial_step, 0)
    arrive_and_forward(4)

    @pl.when(last)
    def _():
        for copy in rims():
            copy.wait()

    def radial_step(k, _):
        y_arrive(k)
        radial(k)

        @pl.when(jnp.logical_and(lax.rem(k, 2) == 1, k < 6))
        def _():
            arrive_and_forward(5 + k // 2)

        return 0

    lax.fori_loop(0, 8, radial_step, 0)

    def out_copy(o):
        rows = pl.ds(o * 8, 8)
        return pltpu.make_async_copy(result.at[:, :, rows, :], out_hbm.at[:, :, rows, :], out_sem.at[o])

    @pl.when(first)
    def _():
        for copy in table_loads():
            copy.wait()
        mine = lax.rem(theta, 2) * 96
        other = 96 - mine
        pairs = ((0, {"theta": sibling}), (4, {"theta": theta_far}), (8, {"theta": sibling}))

        def share(step, o, source, target):
            base, where = pairs[step]
            return pltpu.make_async_remote_copy(
                src_ref=source,
                dst_ref=target,
                send_sem=f_send.at[base + o],
                recv_sem=f_recv.at[base + o],
                device_id=where,
                device_id_type=MESH,
            )

        def step_one(o):
            return share(0, o, part.at[o, pl.ds(pl.multiple_of(other, 8), 96)], half_got.at[o])

        def step_two(o):
            return share(1, o, half_sum.at[o], half_far.at[o])

        def step_three(o):
            return share(2, o, half_total.at[o], half_peer.at[o])

        for o in range(4):
            values = result[:, :, pl.ds(8 * o, 8), :].reshape(192, 256)
            part[o] = jnp.dot(values, table[...], precision=lax.Precision.HIGHEST, preferred_element_type=jnp.float32)
            step_one(o).start()
        for o in range(4):
            step_one(o).wait_recv()
            half_sum[o] = part[o, pl.ds(pl.multiple_of(mine, 8), 96)] + half_got[o]
            step_two(o).start()
        for o in range(4):
            step_two(o).wait_recv()
            half_total[o] = half_sum[o] + half_far[o]
            step_three(o).start()
        order = lax.broadcasted_iota(jnp.int32, (8, 128), 1)
        order = jnp.where(order < KMODES, order, order - KMODES)
        mode_scale = jnp.where(order == 0, 1.0 / NT, 2.0 / NT)
        weights = [jnp.where(order <= cutoff_smem[i], mode_scale, 0.0) for i in range(4)]
        weights = jnp.concatenate(weights * 3, 0)
        even_core = mine == 0
        for o in range(4):
            step_three(o).wait_recv()
            own = half_total[o] * weights
            peer = half_peer[o] * weights
            lower = jnp.where(even_core, own, peer)
            upper = jnp.where(even_core, peer, own)
            coefficients = jnp.concatenate([lower, upper], 0)
            values = jnp.dot(coefficients, table_t[...], precision=lax.Precision.HIGHEST, preferred_element_type=jnp.float32)
            result[:, :, pl.ds(8 * o, 8), :] = values.reshape(6, 4, 8, 256)
            out_copy(o).start()
        for o in range(4):
            step_one(o).wait_send()
            step_two(o).wait_send()
            step_three(o).wait_send()

    @pl.when(jnp.logical_not(first))
    def _():
        for o in range(4):
            out_copy(o).start()

    for copy in t_copies():
        copy.wait_send()
    for copy in z_copies():
        copy.wait_send()
    for k in range(8):

        @pl.when(inner_row)
        def _():
            for copy in x_full(k):
                copy.wait_send()

        @pl.when(jnp.logical_not(inner_row))
        def _():
            for copy in x_last(k):
                copy.wait_send()

        @pl.when(first)
        def _():
            for copy in mirror(k):
                copy.wait_send()

        @pl.when(forwards)
        def _():
            for copy in forward(k):
                copy.wait_send()

    for o in range(4):
        out_copy(o).wait()


def fourier_tables():
    phases = (np.arange(NT)[:, None] * np.arange(KMODES)[None, :]) % NT
    angles = phases.astype(np.float64) * (2.0 * np.pi / NT)
    table = np.concatenate([np.cos(angles), np.sin(angles)], 1).astype(np.float32)
    return table, np.ascontiguousarray(table.reshape(4, 256, 2 * KMODES).transpose(0, 2, 1))


def shards(state_start, state_section, phase, cutoff):
    f32, i32 = jnp.float32, jnp.int32
    table, table_t = fourier_tables()
    anywhere = pl.BlockSpec(memory_space=pltpu.HBM)
    dma = pltpu.SemaphoreType.DMA
    return pl.pallas_call(
        kernel,
        out_shape=jax.ShapeDtypeStruct(state_start.shape, f32),
        in_specs=[anywhere] * 6,
        out_specs=anywhere,
        scratch_shapes=[
            pltpu.VMEM((6, 12, 32, 256), f32),
            pltpu.VMEM((12, 32, 256), i32),
            pltpu.VMEM((6, 4, 32, 256), f32),
            pltpu.VMEM((6, 4, 8, 256), f32),
            pltpu.VMEM((4, 8, 256), i32),
            pltpu.VMEM((6, 4, 8, 256), f32),
            pltpu.VMEM((4, 8, 256), i32),
            pltpu.VMEM((2, 32, 128), f32),
            pltpu.VMEM((2, 32, 128), f32),
            pltpu.VMEM((2, 32, 128), f32),
            pltpu.VMEM((2, 32, 128), f32),
            pltpu.VMEM((256, 2 * KMODES), f32),
            pltpu.VMEM((2 * KMODES, 256), f32),
            pltpu.VMEM((4, 192, 2 * KMODES), f32),
            pltpu.VMEM((4, 96, 2 * KMODES), f32),
            pltpu.VMEM((4, 96, 2 * KMODES), f32),
            pltpu.VMEM((4, 96, 2 * KMODES), f32),
            pltpu.VMEM((4, 96, 2 * KMODES), f32),
            pltpu.VMEM((4, 96, 2 * KMODES), f32),
            pltpu.SMEM((4,), i32),
            dma((8,)),
            dma((8,)),
            dma((6,)),
            dma((4,)),
            dma((16,)),
            dma((16,)),
            dma((16,)),
            dma((16,)),
            dma((16,)),
            dma((4,)),
            dma((4,)),
            dma((2,)),
            dma((2,)),
            dma((12,)),
            dma((12,)),
            dma((4,)),
        ],
        compiler_params=pltpu.CompilerParams(collective_id=0, has_side_effects=True, vmem_limit_bytes=67043328),
        name="jet_section",
    )(state_start, state_section, phase, cutoff, jnp.asarray(table), jnp.asarray(table_t))


def solution(mesh):
    in_specs = (
        P(None, "row", "gz", "theta"),
        P(None, "row", "gz", "theta"),
        P("row", "gz", "theta"),
        P(),
    )
    out_specs = P(None, "row", "gz", "theta")
    return jax.shard_map(shards, mesh=mesh, in_specs=in_specs, out_specs=out_specs, check_vma=False)
```

```python
import functools
import math

import jax
import jax.numpy as jnp
import numpy as np
from jax import lax
from jax.experimental import pallas as pl
from jax.experimental.pallas import tpu as pltpu
from jax.sharding import PartitionSpec as P

NT = 1024
KMODES = 64
GHOST = 3

split_speed = 10.0
time_step = 0.05
weno_epsilon = 1e-06
scaled_epsilon = 4.0 * weno_epsilon * 12.0 / 13.0
side_scale = 3.0 / 13.0

MESH = pl.DeviceIdType.MESH


def primitives(cells, liquid):
    inverse = 1.0 / cells[0]
    kinetic = 0.5 * (cells[1] * cells[1] + cells[2] * cells[2] + cells[3] * cells[3]) * inverse
    internal = cells[4] - kinetic
    pressure = jnp.where(liquid, 3.4 * internal - 4.4 * 0.6, 0.4 * internal)
    return inverse, pressure


def split_flux(cells, velocity, pressure, component, channel):
    flux = cells[channel] * velocity
    if channel == component:
        flux = flux + pressure
    if channel == 4:
        flux = flux + pressure * velocity
    carried = split_speed * cells[channel]
    return flux + carried, flux - carried


def correction(u1, u2, u3, u4, d0, d1, d2, q0, q1, q2):
    a3 = 3.0 * u2
    b3 = 3.0 * u3
    g0 = a3 - u1
    g1 = u2 + u3
    g2 = u4 - b3
    t0 = q0 + (side_scale * g0) * g0
    t1 = q1 + (side_scale * g1) * g1
    t2 = q2 + (side_scale * g2) * g2
    s0 = t0 * t0
    s1 = t1 * t1
    s2 = t2 * t2
    p0 = s1 * s2
    p1 = (6.0 * s0) * s2
    p2 = (3.0 * s0) * s1
    z0 = d0 + d0 + a3
    z1 = g1 + u3
    z2 = b3 - d2
    top = p0 * z0 + p1 * z1 + p2 * z2
    bottom = p0 + p1 + p2
    return (top / bottom) * (1.0 / 6.0)


def line_divergence(upward, downward, axis):
    length = upward.shape[axis]

    def ahead(x, steps):
        return pltpu.roll(x, (-steps) % length, axis)

    def pieces(field):
        u = ahead(field, 1) - field
        um1 = ahead(u, -1)
        um2 = ahead(u, -2)
        up1 = ahead(u, 1)
        d1 = u - um1
        d0 = um1 - um2
        d2 = up1 - u
        return u, um1, um2, up1, d0, d1, d2, d0 * d0 + scaled_epsilon, d1 * d1 + scaled_epsilon, d2 * d2 + scaled_epsilon

    u, um1, um2, up1, d0, d1, d2, q0, q1, q2 = pieces(upward)
    right = upward + correction(um2, um1, u, up1, d0, d1, d2, q0, q1, q2)
    u, um1, um2, up1, d0, d1, d2, q0, q1, q2 = pieces(downward)
    left = downward - correction(up1, u, um1, um2, -d2, -d1, -d0, q2, q1, q0)
    face = right + ahead(left, 1)
    return face - ahead(face, -1)


def kernel(
    start_hbm,
    section_hbm,
    phase_hbm,
    cutoff_hbm,
    table_hbm,
    table_t_hbm,
    out_hbm,
    column,
    column_ph,
    result,
    z_low,
    z_low_ph,
    z_high,
    z_high_ph,
    pack_low,
    pack_high,
    got_low,
    got_high,
    table,
    table_t,
    part,
    half_got,
    half_sum,
    half_far,
    half_total,
    half_peer,
    relay,
    relay_ph,
    cutoff_smem,
    load_sem,
    load_ph_sem,
    rim_sem,
    misc_sem,
    x_send,
    x_recv,
    y_send,
    y_recv,
    m_send,
    r_send,
    r_recv,
    z_send,
    z_recv,
    t_send,
    t_recv,
    f_send,
    f_recv,
    out_sem,
):
    row = lax.axis_index("row")
    theta = lax.axis_index("theta")
    gz = lax.axis_index("gz")
    odd = lax.rem(row, 2)
    partner = row + 1 - 2 * odd
    theta_up = lax.rem(theta + 1, 4)
    theta_down = lax.rem(theta + 3, 4)
    theta_far = lax.rem(theta + 2, 4)
    sibling = theta + 1 - 2 * lax.rem(theta, 2)
    gz_up = lax.rem(gz + 1, 8)
    gz_down = lax.rem(gz + 7, 8)
    first = row == 0
    last = row == 7

    def piece(k):
        octet = k // 2
        half = k % 2
        if isinstance(k, int):
            return pl.ds(octet * 8, 8), pl.ds(half * 128, 128)
        return pl.ds(pl.multiple_of(octet * 8, 8), 8), pl.ds(pl.multiple_of(half * 128, 128), 128)

    def load(k):
        rows, lanes = piece(k)
        return (
            pltpu.make_async_copy(section_hbm.at[:, :, rows, lanes], column.at[:, pl.ds(4, 4), rows, lanes], load_sem.at[k]),
            pltpu.make_async_copy(phase_hbm.at[:, rows, lanes], column_ph.at[pl.ds(4, 4), rows, lanes], load_ph_sem.at[k]),
        )

    for k in range(8):
        for copy in load(k):
            copy.start()
    start_copy = pltpu.make_async_copy(start_hbm, result, misc_sem.at[0])
    start_copy.start()

    def rims():
        copies = []
        for j in range(3):
            copies.append(pltpu.make_async_copy(section_hbm.at[:, pl.ds(3, 1)], column.at[:, pl.ds(8 + j, 1)], rim_sem.at[2 * j]))
            copies.append(pltpu.make_async_copy(phase_hbm.at[pl.ds(3, 1)], column_ph.at[pl.ds(8 + j, 1)], rim_sem.at[2 * j + 1]))
        return copies

    def table_loads():
        return (
            pltpu.make_async_copy(table_hbm.at[pl.ds(pl.multiple_of(theta * 256, 256), 256)], table, misc_sem.at[1]),
            pltpu.make_async_copy(table_t_hbm.at[theta], table_t, misc_sem.at[2]),
            pltpu.make_async_copy(cutoff_hbm, cutoff_smem, misc_sem.at[3]),
        )

    @pl.when(last)
    def _():
        for copy in rims():
            copy.start()

    @pl.when(first)
    def _():
        for copy in table_loads():
            copy.start()

    barrier = pltpu.get_barrier_semaphore()
    for where in (
        {"row": partner},
        {"row": lax.rem(row + 2, 8)},
        {"row": lax.rem(row + 6, 8)},
        {"theta": theta_up},
        {"theta": theta_down},
        {"theta": theta_far},
        {"row": partner, "theta": theta_far},
        {"gz": gz_up},
        {"gz": gz_down},
    ):
        pl.semaphore_signal(barrier, inc=1, device_id=where, device_id_type=MESH)

    def carry(k, source, target, count, send, recv, where):
        rows, lanes = piece(k)
        return (
            pltpu.make_async_remote_copy(
                src_ref=column.at[:, pl.ds(source, count), rows, lanes],
                dst_ref=column.at[:, pl.ds(target, count), rows, lanes],
                send_sem=send.at[k],
                recv_sem=recv.at[k],
                device_id=where,
                device_id_type=MESH,
            ),
            pltpu.make_async_remote_copy(
                src_ref=column_ph.at[pl.ds(source, count), rows, lanes],
                dst_ref=column_ph.at[pl.ds(target, count), rows, lanes],
                send_sem=send.at[k + 8],
                recv_sem=recv.at[k + 8],
                device_id=where,
                device_id_type=MESH,
            ),
        )

    for k in range(8):
        for copy in load(k):
            copy.wait()

    lane = lax.broadcasted_iota(jnp.int32, (8, 128), 1)

    def pack(n, _):
        pair = n // 4
        rows = pl.ds(pl.multiple_of((n % 4) * 8, 8), 8)
        low = jnp.zeros((8, 128), jnp.float32)
        high = jnp.zeros((8, 128), jnp.float32)
        for group in range(14):
            channel, cycle = group % 7, 4 + 2 * pair + group // 7
            if channel < 6:
                near = column[channel, cycle, rows, pl.ds(0, 128)]
                far = column[channel, cycle, rows, pl.ds(128, 128)]
            else:
                near = column_ph[cycle, rows, pl.ds(0, 128)].astype(jnp.float32)
                far = column_ph[cycle, rows, pl.ds(128, 128)].astype(jnp.float32)
            if group:
                near = pltpu.roll(near, 8 * group, 1)
            far = pltpu.roll(far, (8 * group + 8) % 128, 1)
            here = lane // 8 == group
            low = jnp.where(here, near, low)
            high = jnp.where(here, far, high)
        pack_low[pair, rows, :] = low
        pack_high[pair, rows, :] = high
        return 0

    lax.fori_loop(0, 8, pack, 0)

    inner_row = jnp.logical_and(row > 0, row < 7)
    to_partner = {"row": partner}

    def x_full(k):
        return carry(k, 4, 8 * odd, 4, x_send, x_recv, to_partner)

    def x_first(k):
        return carry(k, 5, 1, 3, x_send, x_recv, to_partner)

    def x_last(k):
        return carry(k, 4, 8, 3, x_send, x_recv, to_partner)

    def mirror(k):
        return carry(k, 4, 1, 3, m_send, y_recv, {"theta": theta_far})

    def forward(k):
        target = jnp.where(odd == 1, lax.rem(row + 6, 8), lax.rem(row + 2, 8))
        return carry(k, 9 - 9 * odd, 1 + 7 * odd, 3, y_send, y_recv, {"row": target})

    def relay_copies(j, out):
        rows = pl.ds((j // 2) * 8, 8)
        column_rows, lanes = piece(j + 4)
        if out:
            return (
                pltpu.make_async_remote_copy(
                    src_ref=column.at[:, pl.ds(5, 3), column_rows, lanes],
                    dst_ref=relay.at[:, :, rows, lanes],
                    send_sem=x_send.at[j + 4],
                    recv_sem=r_recv.at[j],
                    device_id={"row": partner, "theta": theta_far},
                    device_id_type=MESH,
                ),
                pltpu.make_async_remote_copy(
                    src_ref=column_ph.at[pl.ds(5, 3), column_rows, lanes],
                    dst_ref=relay_ph.at[:, rows, lanes],
                    send_sem=x_send.at[j + 12],
                    recv_sem=r_recv.at[j + 4],
                    device_id={"row": partner, "theta": theta_far},
                    device_id_type=MESH,
                ),
            )
        return (
            pltpu.make_async_remote_copy(
                src_ref=relay.at[:, :, rows, lanes],
                dst_ref=column.at[:, pl.ds(1, 3), column_rows, lanes],
                send_sem=r_send.at[j],
                recv_sem=x_recv.at[j + 4],
                device_id={"theta": theta_far},
                device_id_type=MESH,
            ),
            pltpu.make_async_remote_copy(
                src_ref=relay_ph.at[:, rows, lanes],
                dst_ref=column_ph.at[pl.ds(1, 3), column_rows, lanes],
                send_sem=r_send.at[j + 4],
                recv_sem=x_recv.at[j + 12],
                device_id={"theta": theta_far},
                device_id_type=MESH,
            ),
        )

    def hand_over(j):
        @pl.when(row == 1)
        def _():
            for copy in relay_copies(j, True):
                copy.wait_recv()
            for copy in relay_copies(j, False):
                copy.start()

    forwards = jnp.logical_or(jnp.logical_and(odd == 0, row < 6), jnp.logical_and(odd == 1, row > 1))

    def z_copies():
        copies = []
        for side, (rows, cells_to, phase_to, where) in enumerate(
            (
                (pl.ds(0, 8), z_high, z_high_ph, {"gz": gz_down}),
                (pl.ds(24, 8), z_low, z_low_ph, {"gz": gz_up}),
            )
        ):
            copies.append(
                pltpu.make_async_remote_copy(
                    src_ref=column.at[:, pl.ds(4, 4), rows, :],
                    dst_ref=cells_to,
                    send_sem=z_send.at[2 * side],
                    recv_sem=z_recv.at[2 * side],
                    device_id=where,
                    device_id_type=MESH,
                )
            )
            copies.append(
                pltpu.make_async_remote_copy(
                    src_ref=column_ph.at[pl.ds(4, 4), rows, :],
                    dst_ref=phase_to,
                    send_sem=z_send.at[2 * side + 1],
                    recv_sem=z_recv.at[2 * side + 1],
                    device_id=where,
                    device_id_type=MESH,
                )
            )
        return copies

    def t_copies():
        return (
            pltpu.make_async_remote_copy(
                src_ref=pack_low,
                dst_ref=got_high,
                send_sem=t_send.at[0],
                recv_sem=t_recv.at[0],
                device_id={"theta": theta_down},
                device_id_type=MESH,
            ),
            pltpu.make_async_remote_copy(
                src_ref=pack_high,
                dst_ref=got_low,
                send_sem=t_send.at[1],
                recv_sem=t_recv.at[1],
                device_id={"theta": theta_up},
                device_id_type=MESH,
            ),
        )

    pl.semaphore_wait(barrier, 9)
    for copy in t_copies():
        copy.start()
    for copy in z_copies():
        copy.start()

    @pl.when(inner_row)
    def _():
        for k in range(8):
            for copy in x_full(k):
                copy.start()

    @pl.when(first)
    def _():
        for k in range(8):
            for copy in mirror(k):
                copy.start()
            if k < 4:
                for copy in relay_copies(k, True):
                    copy.start()
        for k in range(4):
            for copy in x_first(k):
                copy.start()

    @pl.when(last)
    def _():
        for k in range(8):
            for copy in x_last(k):
                copy.start()

    start_copy.wait()
    for copy in t_copies():
        copy.wait_recv()

    quarter = 0.25 * time_step

    def azimuthal(n, _):
        cycle = n // 4
        octet = n % 4
        rows = pl.ds(pl.multiple_of(octet * 8, 8), 8)
        pair = cycle // 2
        low = got_low[pair, rows, :]
        high = got_high[pair, rows, :]
        base = lax.rem(cycle, 2) * 56

        def edge(channel):
            offset = base + 8 * channel
            upper = pltpu.roll(high, lax.rem(128 - offset, 128), 1)
            lower = pltpu.roll(low, 120 - offset, 1)
            return jnp.where(lane < 64, upper, lower)

        cells = [jnp.concatenate([column[c, 4 + cycle, rows, :], edge(c)], 1) for c in range(6)]
        old = [result[c, cycle, rows, :] for c in range(6)]
        new = []
        material = jnp.concatenate([column_ph[4 + cycle, rows, :].astype(jnp.float32), edge(6)], 1)
        inverse, pressure = primitives(cells, material > 0.5)
        velocity = cells[2] * inverse
        radius = (row * 4 + cycle).astype(jnp.float32) + 0.5
        scale = 0.5 * quarter / (radius * (2.0 * math.pi / NT))
        source_scale = quarter / radius
        for c in range(6):
            upward, downward = split_flux(cells, velocity, pressure, 2, c)
            change = line_divergence(upward, downward, 1)[:, :256] * scale
            value = 0.75 * old[c] + 0.25 * cells[c][:, :256] - change
            if c == 1:
                value = value + source_scale * (cells[2] * velocity + pressure)[:, :256]
            if c == 2:
                value = value - source_scale * (cells[1] * velocity)[:, :256]
            new.append(value)
        for c in range(6):
            result[c, cycle, rows, :] = new[c]
        return 0

    row8 = lax.broadcasted_iota(jnp.int32, (8, 128), 0)

    def axial(n):
        cycle = n // 2
        lanes = pl.ds(pl.multiple_of((n % 2) * 128, 128), 128)
        cells = [
            jnp.concatenate(
                [column[c, 4 + cycle, :, lanes], jnp.where(row8 < 4, z_high[c, cycle, :, lanes], z_low[c, cycle, :, lanes])], 0
            )
            for c in range(6)
        ]
        material = jnp.concatenate(
            [column_ph[4 + cycle, :, lanes], jnp.where(row8 < 4, z_high_ph[cycle, :, lanes], z_low_ph[cycle, :, lanes])], 0
        )
        inverse, pressure = primitives(cells, material == 1)
        velocity = cells[3] * inverse
        for c in range(6):
            upward, downward = split_flux(cells, velocity, pressure, 3, c)
            change = line_divergence(upward, downward, 0)[:32] * (0.5 * quarter)
            result[c, cycle, :, lanes] = result[c, cycle, :, lanes] - change

    def arrive_and_forward(k):
        @pl.when(forwards)
        def _():
            for copy in carry(k, 4, 4, 4, x_send, x_recv, to_partner):
                copy.wait_recv()
            for copy in forward(k):
                copy.start()

    def x_arrive(k):
        @pl.when(jnp.logical_not(forwards))
        def _():
            for copy in carry(k, 4, 4, 3, x_send, x_recv, to_partner):
                copy.wait_recv()

    def y_arrive(k):
        @pl.when(row != 7)
        def _():
            for copy in carry(k, 4, 4, 3, y_send, y_recv, to_partner):
                copy.wait_recv()

    flip = jnp.where(first, -1.0, 1.0)

    def radial(k):
        rows, lanes = piece(k)
        planes = [jnp.where(first, 4 - p, p) for p in (1, 2, 3)] + list(range(4, 11))
        stack = []
        for i, plane in enumerate(planes):
            cells = [column[c, plane, rows, lanes] for c in range(6)]
            if i < 3:
                cells[1] = cells[1] * flip
                cells[2] = cells[2] * flip
            inverse, pressure = primitives(cells, column_ph[plane, rows, lanes] == 1)
            stack.append((cells, cells[1] * inverse, pressure))
        for c in range(6):
            up, down = zip(*[split_flux(cells, v, p, 1, c) for cells, v, p in stack])

            def pieces(field):
                u = [field[i + 1] - field[i] for i in range(9)]
                d = [None] + [u[i] - u[i - 1] for i in range(1, 9)]
                q = [None] + [d[i] * d[i] + scaled_epsilon for i in range(1, 9)]
                return u, d, q

            u, d, q = pieces(up)
            right = [
                up[i] + correction(u[i - 2], u[i - 1], u[i], u[i + 1], d[i - 1], d[i], d[i + 1], q[i - 1], q[i], q[i + 1])
                for i in range(2, 7)
            ]
            u, d, q = pieces(down)
            left = [
                down[i] - correction(u[i + 1], u[i], u[i - 1], u[i - 2], -d[i + 1], -d[i], -d[i - 1], q[i + 1], q[i], q[i - 1])
                for i in range(3, 8)
            ]
            face = [a + b for a, b in zip(right, left)]
            weighted = [(row * 4 + j).astype(jnp.float32) * face[j] for j in range(5)]
            for j in range(4):
                radius = (row * 4 + j).astype(jnp.float32) + 0.5
                result[c, j, rows, lanes] = result[c, j, rows, lanes] - (weighted[j + 1] - weighted[j]) * (0.5 * quarter / radius)

    def axial_step(n, _):
        axial(n)
        return 0

    lax.fori_loop(0, 8, azimuthal, 0)
    arrive_and_forward(0)
    lax.fori_loop(8, 12, azimuthal, 0)
    arrive_and_forward(1)
    hand_over(0)
    lax.fori_loop(12, 16, azimuthal, 0)
    arrive_and_forward(2)
    hand_over(1)
    for copy in z_copies():
        copy.wait_recv()
    lax.fori_loop(0, 4, axial_step, 0)
    arrive_and_forward(3)
    hand_over(2)
    lax.fori_loop(4, 8, axial_step, 0)
    arrive_and_forward(4)
    hand_over(3)

    @pl.when(last)
    def _():
        for copy in rims():
            copy.wait()

    def tile(o):
        return pl.ds(o * 8, 8) if isinstance(o, int) else pl.ds(pl.multiple_of(o * 8, 8), 8)

    def out_copy(o):
        return pltpu.make_async_copy(result.at[:, :, tile(o), :], out_hbm.at[:, :, tile(o), :], out_sem.at[o])

    mine = pl.multiple_of(lax.rem(theta, 2) * 96, 8)
    other = pl.multiple_of(96 - lax.rem(theta, 2) * 96, 8)

    def share(step, o, source, target, where):
        return pltpu.make_async_remote_copy(
            src_ref=source,
            dst_ref=target,
            send_sem=f_send.at[4 * step + o],
            recv_sem=f_recv.at[4 * step + o],
            device_id={"theta": where},
            device_id_type=MESH,
        )

    def step_one(o):
        return share(0, o, part.at[o, pl.ds(other, 96)], half_got.at[o], sibling)

    def step_two(o):
        return share(1, o, half_sum.at[o], half_far.at[o], theta_far)

    def step_three(o):
        return share(2, o, half_total.at[o], half_peer.at[o], sibling)

    def filter_one(o):
        values = result[:, :, tile(o), :].reshape(192, 256)
        part[o] = jnp.dot(values, table[...], precision=lax.Precision.HIGHEST, preferred_element_type=jnp.float32)
        step_one(o).start()

    def filter_two(o):
        step_one(o).wait_recv()
        half_sum[o] = part[o, pl.ds(mine, 96)] + half_got[o]
        step_two(o).start()

    def filter_three(o):
        step_two(o).wait_recv()
        half_total[o] = half_sum[o] + half_far[o]
        step_three(o).start()

    def filter_last(o, _):
        order = lax.broadcasted_iota(jnp.int32, (8, 128), 1)
        order = jnp.where(order < KMODES, order, order - KMODES)
        mode_scale = jnp.where(order == 0, 1.0 / NT, 2.0 / NT)
        weights = [jnp.where(order <= cutoff_smem[i], mode_scale, 0.0) for i in range(4)]
        weights = jnp.concatenate(weights * 3, 0)
        even_core = lax.rem(theta, 2) == 0
        step_three(o).wait_recv()
        own = half_total[o] * weights
        peer = half_peer[o] * weights
        lower = jnp.where(even_core, own, peer)
        upper = jnp.where(even_core, peer, own)
        coefficients = jnp.concatenate([lower, upper], 0)
        values = jnp.dot(coefficients, table_t[...], precision=lax.Precision.HIGHEST, preferred_element_type=jnp.float32)
        result[:, :, tile(o), :] = values.reshape(6, 4, 8, 256)
        out_copy(o).start()
        return 0

    @pl.when(first)
    def _():
        for copy in table_loads():
            copy.wait()

    def radial_step(k, _):
        x_arrive(k)
        y_arrive(k)
        radial(k)
        o = k // 2
        whole = lax.rem(k, 2) == 1

        @pl.when(jnp.logical_and(whole, k < 6))
        def _():
            arrive_and_forward(5 + o)

        @pl.when(jnp.logical_and(whole, first))
        def _():
            filter_one(o)

            @pl.when(o > 0)
            def _():
                filter_two(o - 1)

        @pl.when(jnp.logical_and(whole, jnp.logical_not(first)))
        def _():
            out_copy(o).start()

        return 0

    lax.fori_loop(0, 8, radial_step, 0)

    @pl.when(first)
    def _():
        filter_two(3)
        for o in range(3):
            filter_three(o)
        lax.fori_loop(0, 3, filter_last, 0)
        filter_three(3)
        lax.fori_loop(3, 4, filter_last, 0)
        for o in range(4):
            step_one(o).wait_send()
            step_two(o).wait_send()
            step_three(o).wait_send()

    for copy in t_copies():
        copy.wait_send()
    for copy in z_copies():
        copy.wait_send()
    for k in range(8):

        @pl.when(inner_row)
        def _():
            for copy in x_full(k):
                copy.wait_send()

        @pl.when(jnp.logical_not(inner_row))
        def _():
            for copy in x_last(k):
                copy.wait_send()

        @pl.when(first)
        def _():
            for copy in mirror(k):
                copy.wait_send()

        @pl.when(forwards)
        def _():
            for copy in forward(k):
                copy.wait_send()

    @pl.when(row == 1)
    def _():
        for j in range(4):
            for copy in relay_copies(j, False):
                copy.wait_send()

    for o in range(4):
        out_copy(o).wait()


def fourier_tables():
    phases = (np.arange(NT)[:, None] * np.arange(KMODES)[None, :]) % NT
    angles = phases.astype(np.float64) * (2.0 * np.pi / NT)
    table = np.concatenate([np.cos(angles), np.sin(angles)], 1).astype(np.float32)
    return table, np.ascontiguousarray(table.reshape(4, 256, 2 * KMODES).transpose(0, 2, 1))


def shards(state_start, state_section, phase, cutoff):
    f32, i32 = jnp.float32, jnp.int32
    table, table_t = fourier_tables()
    anywhere = pl.BlockSpec(memory_space=pltpu.HBM)
    dma = pltpu.SemaphoreType.DMA
    return pl.pallas_call(
        kernel,
        out_shape=jax.ShapeDtypeStruct(state_start.shape, f32),
        in_specs=[anywhere] * 6,
        out_specs=anywhere,
        scratch_shapes=[
            pltpu.VMEM((6, 12, 32, 256), f32),
            pltpu.VMEM((12, 32, 256), i32),
            pltpu.VMEM((6, 4, 32, 256), f32),
            pltpu.VMEM((6, 4, 8, 256), f32),
            pltpu.VMEM((4, 8, 256), i32),
            pltpu.VMEM((6, 4, 8, 256), f32),
            pltpu.VMEM((4, 8, 256), i32),
            pltpu.VMEM((2, 32, 128), f32),
            pltpu.VMEM((2, 32, 128), f32),
            pltpu.VMEM((2, 32, 128), f32),
            pltpu.VMEM((2, 32, 128), f32),
            pltpu.VMEM((256, 2 * KMODES), f32),
            pltpu.VMEM((2 * KMODES, 256), f32),
            pltpu.VMEM((4, 192, 2 * KMODES), f32),
            pltpu.VMEM((4, 96, 2 * KMODES), f32),
            pltpu.VMEM((4, 96, 2 * KMODES), f32),
            pltpu.VMEM((4, 96, 2 * KMODES), f32),
            pltpu.VMEM((4, 96, 2 * KMODES), f32),
            pltpu.VMEM((4, 96, 2 * KMODES), f32),
            pltpu.VMEM((6, 3, 16, 256), f32),
            pltpu.VMEM((3, 16, 256), i32),
            pltpu.SMEM((4,), i32),
            dma((8,)),
            dma((8,)),
            dma((6,)),
            dma((4,)),
            dma((16,)),
            dma((16,)),
            dma((16,)),
            dma((16,)),
            dma((16,)),
            dma((8,)),
            dma((8,)),
            dma((4,)),
            dma((4,)),
            dma((2,)),
            dma((2,)),
            dma((12,)),
            dma((12,)),
            dma((4,)),
        ],
        compiler_params=pltpu.CompilerParams(collective_id=0, has_side_effects=True, vmem_limit_bytes=67043328),
        name="jet_section",
    )(state_start, state_section, phase, cutoff, jnp.asarray(table), jnp.asarray(table_t))


def solution(mesh):
    in_specs = (
        P(None, "row", "gz", "theta"),
        P(None, "row", "gz", "theta"),
        P("row", "gz", "theta"),
        P(),
    )
    out_specs = P(None, "row", "gz", "theta")
    return jax.shard_map(shards, mesh=mesh, in_specs=in_specs, out_specs=out_specs, check_vma=False)
```

```python
import functools
import math

import jax
import jax.numpy as jnp
import numpy as np
from jax import lax
from jax.experimental import pallas as pl
from jax.experimental.pallas import tpu as pltpu
from jax.sharding import PartitionSpec as P

NT = 1024
KMODES = 64
DIRECT = 3

split_speed = 10.0
time_step = 0.05
weno_epsilon = 1e-06
scaled_epsilon = 4.0 * weno_epsilon * 12.0 / 13.0
side_scale = 3.0 / 13.0

MESH = pl.DeviceIdType.MESH


def primitives(cells, liquid):
    inverse = 1.0 / cells[0]
    kinetic = 0.5 * (cells[1] * cells[1] + cells[2] * cells[2] + cells[3] * cells[3]) * inverse
    internal = cells[4] - kinetic
    pressure = jnp.where(liquid, 3.4 * internal - 4.4 * 0.6, 0.4 * internal)
    return inverse, pressure


def split_flux(cells, velocity, pressure, component, channel):
    flux = cells[channel] * velocity
    if channel == component:
        flux = flux + pressure
    if channel == 4:
        flux = flux + pressure * velocity
    carried = split_speed * cells[channel]
    return flux + carried, flux - carried


def correction(u1, u2, u3, u4, d0, d1, d2, q0, q1, q2):
    a3 = 3.0 * u2
    b3 = 3.0 * u3
    g0 = a3 - u1
    g1 = u2 + u3
    g2 = u4 - b3
    t0 = q0 + (side_scale * g0) * g0
    t1 = q1 + (side_scale * g1) * g1
    t2 = q2 + (side_scale * g2) * g2
    s0 = t0 * t0
    s1 = t1 * t1
    s2 = t2 * t2
    p0 = s1 * s2
    p1 = (6.0 * s0) * s2
    p2 = (3.0 * s0) * s1
    z0 = d0 + d0 + a3
    z1 = g1 + u3
    z2 = b3 - d2
    top = p0 * z0 + p1 * z1 + p2 * z2
    bottom = p0 + p1 + p2
    return (top / bottom) * (1.0 / 6.0)


def line_divergence(upward, downward, axis):
    length = upward.shape[axis]

    def ahead(x, steps):
        return pltpu.roll(x, (-steps) % length, axis)

    def pieces(field):
        u = ahead(field, 1) - field
        um1 = ahead(u, -1)
        um2 = ahead(u, -2)
        up1 = ahead(u, 1)
        d1 = u - um1
        d0 = um1 - um2
        d2 = up1 - u
        return u, um1, um2, up1, d0, d1, d2, d0 * d0 + scaled_epsilon, d1 * d1 + scaled_epsilon, d2 * d2 + scaled_epsilon

    u, um1, um2, up1, d0, d1, d2, q0, q1, q2 = pieces(upward)
    right = upward + correction(um2, um1, u, up1, d0, d1, d2, q0, q1, q2)
    u, um1, um2, up1, d0, d1, d2, q0, q1, q2 = pieces(downward)
    left = downward - correction(up1, u, um1, um2, -d2, -d1, -d0, q2, q1, q0)
    face = right + ahead(left, 1)
    return face - ahead(face, -1)


def product(values, high_ref, low_ref):
    high = values.astype(jnp.bfloat16)
    low = (values - high.astype(jnp.float32)).astype(jnp.bfloat16)
    dot = functools.partial(jnp.dot, preferred_element_type=jnp.float32)
    return dot(high, high_ref[...]) + (dot(low, high_ref[...]) + dot(high, low_ref[...]))


def kernel(
    start_hbm,
    section_hbm,
    phase_hbm,
    cutoff_hbm,
    table_hbm,
    table_low_hbm,
    table_t_hbm,
    table_t_low_hbm,
    out_hbm,
    column,
    column_ph,
    result,
    z_low,
    z_low_ph,
    z_high,
    z_high_ph,
    pack_low,
    pack_high,
    got_low,
    got_high,
    table,
    table_low,
    table_t,
    table_t_low,
    part,
    half_got,
    half_sum,
    half_far,
    half_total,
    half_peer,
    relay,
    relay_ph,
    cutoff_smem,
    load_sem,
    load_ph_sem,
    rim_sem,
    misc_sem,
    x_send,
    x_recv,
    b_send,
    b_recv,
    y_send,
    y_recv,
    c_recv,
    m_send,
    r_send,
    r_recv,
    z_send,
    z_recv,
    t_send,
    t_recv,
    f_send,
    f_recv,
    out_sem,
):
    row = lax.axis_index("row")
    theta = lax.axis_index("theta")
    gz = lax.axis_index("gz")
    odd = lax.rem(row, 2)
    partner = row + 1 - 2 * odd
    theta_up = lax.rem(theta + 1, 4)
    theta_down = lax.rem(theta + 3, 4)
    theta_far = lax.rem(theta + 2, 4)
    sibling = theta + 1 - 2 * lax.rem(theta, 2)
    gz_up = lax.rem(gz + 1, 8)
    gz_down = lax.rem(gz + 7, 8)
    first = row == 0
    last = row == 7

    def piece(k):
        octet = k // 2
        half = k % 2
        if isinstance(k, int):
            return pl.ds(octet * 8, 8), pl.ds(half * 128, 128)
        return pl.ds(pl.multiple_of(octet * 8, 8), 8), pl.ds(pl.multiple_of(half * 128, 128), 128)

    def load(k):
        rows, lanes = piece(k)
        return (
            pltpu.make_async_copy(section_hbm.at[:, :, rows, lanes], column.at[:, pl.ds(4, 4), rows, lanes], load_sem.at[k]),
            pltpu.make_async_copy(phase_hbm.at[:, rows, lanes], column_ph.at[pl.ds(4, 4), rows, lanes], load_ph_sem.at[k]),
        )

    for k in range(8):
        for copy in load(k):
            copy.start()
    start_copy = pltpu.make_async_copy(start_hbm, result, misc_sem.at[0])
    start_copy.start()

    def rims():
        copies = []
        for j in range(3):
            copies.append(pltpu.make_async_copy(section_hbm.at[:, pl.ds(3, 1)], column.at[:, pl.ds(8 + j, 1)], rim_sem.at[2 * j]))
            copies.append(pltpu.make_async_copy(phase_hbm.at[pl.ds(3, 1)], column_ph.at[pl.ds(8 + j, 1)], rim_sem.at[2 * j + 1]))
        return copies

    def table_loads():
        return (
            pltpu.make_async_copy(table_hbm.at[theta], table, misc_sem.at[1]),
            pltpu.make_async_copy(table_t_hbm.at[theta], table_t, misc_sem.at[2]),
            pltpu.make_async_copy(table_low_hbm.at[theta], table_low, misc_sem.at[4]),
            pltpu.make_async_copy(table_t_low_hbm.at[theta], table_t_low, misc_sem.at[5]),
            pltpu.make_async_copy(cutoff_hbm, cutoff_smem, misc_sem.at[3]),
        )

    @pl.when(last)
    def _():
        for copy in rims():
            copy.start()

    @pl.when(first)
    def _():
        for copy in table_loads():
            copy.start()

    barrier = pltpu.get_barrier_semaphore()
    for where in (
        {"row": partner},
        {"row": lax.rem(row + 2, 8)},
        {"row": lax.rem(row + 6, 8)},
        {"theta": theta_up},
        {"theta": theta_down},
        {"theta": theta_far},
        {"row": partner, "theta": theta_far},
        {"gz": gz_up},
        {"gz": gz_down},
    ):
        pl.semaphore_signal(barrier, inc=1, device_id=where, device_id_type=MESH)

    def carry(k, source, target, count, send, recv, where):
        rows, lanes = piece(k)
        return (
            pltpu.make_async_remote_copy(
                src_ref=column.at[:, pl.ds(source, count), rows, lanes],
                dst_ref=column.at[:, pl.ds(target, count), rows, lanes],
                send_sem=send.at[k],
                recv_sem=recv.at[k],
                device_id=where,
                device_id_type=MESH,
            ),
            pltpu.make_async_remote_copy(
                src_ref=column_ph.at[pl.ds(source, count), rows, lanes],
                dst_ref=column_ph.at[pl.ds(target, count), rows, lanes],
                send_sem=send.at[k + 8],
                recv_sem=recv.at[k + 8],
                device_id=where,
                device_id_type=MESH,
            ),
        )

    for k in range(8):
        for copy in load(k):
            copy.wait()

    lane = lax.broadcasted_iota(jnp.int32, (8, 128), 1)

    def pack(n, _):
        rows = pl.ds(pl.multiple_of(n * 8, 8), 8)
        low = jnp.zeros((8, 128), jnp.float32)
        high = jnp.zeros((8, 128), jnp.float32)
        for group in range(28):
            channel, cycle = group % 7, 4 + group // 7
            if channel < 6:
                near = column[channel, cycle, rows, pl.ds(0, 128)]
                far = column[channel, cycle, rows, pl.ds(128, 128)]
            else:
                near = column_ph[cycle, rows, pl.ds(0, 128)].astype(jnp.float32)
                far = column_ph[cycle, rows, pl.ds(128, 128)].astype(jnp.float32)
            if group:
                near = pltpu.roll(near, 4 * group, 1)
            far = pltpu.roll(far, (4 * group + 4) % 128, 1)
            here = lane // 4 == group
            low = jnp.where(here, near, low)
            high = jnp.where(here, far, high)
        pack_low[rows, :] = low
        pack_high[rows, :] = high
        return 0

    lax.fori_loop(0, 4, pack, 0)

    inner_row = jnp.logical_and(row > 0, row < 7)
    to_partner = {"row": partner}

    swapped = jnp.logical_and(odd == 1, inner_row) & (row > 1)

    def x_three(k):
        return carry(k, jnp.where(swapped, 5, 4), jnp.where(swapped, 9, 8 * odd), 3, x_send, x_recv, to_partner)

    def x_fourth(k):
        return carry(k, jnp.where(swapped, 4, 7), jnp.where(swapped, 8, 3 + 8 * odd), 1, b_send, b_recv, to_partner)

    def x_first(k):
        return carry(k, 5, 1, 3, x_send, x_recv, to_partner)

    def mirror(k):
        return carry(k, 4, 1, 3, m_send, y_recv, {"theta": theta_far})

    def forward(k):
        target = jnp.where(odd == 1, lax.rem(row + 6, 8), lax.rem(row + 2, 8))
        return carry(k, 9 - 9 * odd, 1 + 7 * odd, 3, y_send, y_recv, {"row": target})

    def forward_two(k):
        return carry(k, 9, 1, 2, y_send, y_recv, {"row": 2})

    def arrival(k, count, recv):
        return carry(k, 4, 4, count, x_send, recv, to_partner)

    def through(k, source, source_ph, target, target_ph, send, recv, where):
        rows, lanes = piece(k)
        return (
            pltpu.make_async_remote_copy(
                src_ref=source.at[:, :, rows, lanes],
                dst_ref=target.at[:, :, rows, lanes],
                send_sem=send.at[k],
                recv_sem=recv.at[k],
                device_id=where,
                device_id_type=MESH,
            ),
            pltpu.make_async_remote_copy(
                src_ref=source_ph.at[:, rows, lanes],
                dst_ref=target_ph.at[:, rows, lanes],
                send_sem=send.at[k + 8],
                recv_sem=recv.at[k + 8],
                device_id=where,
                device_id_type=MESH,
            ),
        )

    def planes_of(start, count):
        return column.at[:, pl.ds(start, count)], column_ph.at[pl.ds(start, count)]

    one_plane = relay.at[:, pl.ds(0, 1)], relay_ph.at[pl.ds(0, 1)]

    def relay_out(k):
        return through(k, *planes_of(5, 3), relay, relay_ph, x_send, r_recv, {"row": partner, "theta": theta_far})

    def relay_on(k):
        return through(k, relay, relay_ph, *planes_of(1, 3), r_send, x_recv, {"theta": theta_far})

    def fourth_out(k):
        return through(k, *planes_of(7, 1), *one_plane, b_send, r_recv, {"row": 3})

    def fourth_on(k):
        return through(k, *one_plane, *planes_of(3, 1), r_send, c_recv, {"row": 2})

    def hand_over():
        @pl.when(row == 1)
        def _():
            for k in range(DIRECT, 8):
                for copy in relay_out(k):
                    copy.wait_recv()
                for copy in relay_on(k):
                    copy.start()

        @pl.when(row == 3)
        def _():
            for k in range(8):
                for copy in fourth_out(k):
                    copy.wait_recv()
                for copy in fourth_on(k):
                    copy.start()

    forwards = jnp.logical_or(jnp.logical_and(odd == 0, row < 6), jnp.logical_and(odd == 1, row > 1))

    def z_copies():
        copies = []
        for side, (rows, cells_to, phase_to, where) in enumerate(
            (
                (pl.ds(0, 8), z_high, z_high_ph, {"gz": gz_down}),
                (pl.ds(24, 8), z_low, z_low_ph, {"gz": gz_up}),
            )
        ):
            copies.append(
                pltpu.make_async_remote_copy(
                    src_ref=column.at[:, pl.ds(4, 4), rows, :],
                    dst_ref=cells_to,
                    send_sem=z_send.at[2 * side],
                    recv_sem=z_recv.at[2 * side],
                    device_id=where,
                    device_id_type=MESH,
                )
            )
            copies.append(
                pltpu.make_async_remote_copy(
                    src_ref=column_ph.at[pl.ds(4, 4), rows, :],
                    dst_ref=phase_to,
                    send_sem=z_send.at[2 * side + 1],
                    recv_sem=z_recv.at[2 * side + 1],
                    device_id=where,
                    device_id_type=MESH,
                )
            )
        return copies

    def t_copies():
        return (
            pltpu.make_async_remote_copy(
                src_ref=pack_low,
                dst_ref=got_high,
                send_sem=t_send.at[0],
                recv_sem=t_recv.at[0],
                device_id={"theta": theta_down},
                device_id_type=MESH,
            ),
            pltpu.make_async_remote_copy(
                src_ref=pack_high,
                dst_ref=got_low,
                send_sem=t_send.at[1],
                recv_sem=t_recv.at[1],
                device_id={"theta": theta_up},
                device_id_type=MESH,
            ),
        )

    pl.semaphore_wait(barrier, 9)
    for copy in t_copies():
        copy.start()
    for copy in z_copies():
        copy.start()

    @pl.when(inner_row)
    def _():
        for k in range(8):
            for copy in x_three(k):
                copy.start()

        @pl.when(row > 1)
        def _():
            for k in range(8):
                for copy in x_fourth(k):
                    copy.start()

        @pl.when(row == 1)
        def _():
            for k in range(8):
                for copy in fourth_out(k):
                    copy.start()

    @pl.when(first)
    def _():
        for k in range(8):
            for copy in mirror(k):
                copy.start()
            if k >= DIRECT:
                for copy in relay_out(k):
                    copy.start()
        for k in range(DIRECT):
            for copy in x_first(k):
                copy.start()

    @pl.when(last)
    def _():
        for k in range(8):
            for copy in x_three(k):
                copy.start()

    start_copy.wait()
    for copy in t_copies():
        copy.wait_recv()

    quarter = 0.25 * time_step

    lane16 = lax.broadcasted_iota(jnp.int32, (16, 128), 1)

    def azimuthal(n, _):
        cycle = n // 2
        rows = pl.ds(pl.multiple_of((n % 2) * 16, 8), 16)
        low = got_low[rows, :]
        high = got_high[rows, :]
        base = cycle * 28

        def edge(channel):
            offset = base + 4 * channel
            upper = pltpu.roll(high, lax.rem(128 - offset, 128), 1)
            lower = pltpu.roll(low, 124 - offset, 1)
            return jnp.where(lane16 < 64, upper, lower)

        cells = [jnp.concatenate([column[c, 4 + cycle, rows, :], edge(c)], 1) for c in range(6)]
        old = [result[c, cycle, rows, :] for c in range(6)]
        new = []
        material = jnp.concatenate([column_ph[4 + cycle, rows, :].astype(jnp.float32), edge(6)], 1)
        inverse, pressure = primitives(cells, material > 0.5)
        velocity = cells[2] * inverse
        radius = (row * 4 + cycle).astype(jnp.float32) + 0.5
        scale = 0.5 * quarter / (radius * (2.0 * math.pi / NT))
        source_scale = quarter / radius
        for c in range(6):
            upward, downward = split_flux(cells, velocity, pressure, 2, c)
            change = line_divergence(upward, downward, 1)[:, :256] * scale
            value = 0.75 * old[c] + 0.25 * cells[c][:, :256] - change
            if c == 1:
                value = value + source_scale * (cells[2] * velocity + pressure)[:, :256]
            if c == 2:
                value = value - source_scale * (cells[1] * velocity)[:, :256]
            new.append(value)
        for c in range(6):
            result[c, cycle, rows, :] = new[c]
        return 0

    row8 = lax.broadcasted_iota(jnp.int32, (8, 128), 0)

    def axial(n):
        cycle = n // 2
        lanes = pl.ds(pl.multiple_of((n % 2) * 128, 128), 128)
        cells = [
            jnp.concatenate(
                [column[c, 4 + cycle, :, lanes], jnp.where(row8 < 4, z_high[c, cycle, :, lanes], z_low[c, cycle, :, lanes])], 0
            )
            for c in range(6)
        ]
        material = jnp.concatenate(
            [column_ph[4 + cycle, :, lanes], jnp.where(row8 < 4, z_high_ph[cycle, :, lanes], z_low_ph[cycle, :, lanes])], 0
        )
        inverse, pressure = primitives(cells, material == 1)
        velocity = cells[3] * inverse
        for c in range(6):
            upward, downward = split_flux(cells, velocity, pressure, 3, c)
            change = line_divergence(upward, downward, 0)[:32] * (0.5 * quarter)
            result[c, cycle, :, lanes] = result[c, cycle, :, lanes] - change

    def arrive_and_forward(k):
        @pl.when(forwards)
        def _():
            for copy in arrival(k, 3, x_recv):
                copy.wait_recv()

        @pl.when(jnp.logical_and(forwards, row > 0))
        def _():
            for copy in forward(k):
                copy.start()

        @pl.when(first)
        def _():
            for copy in forward_two(k):
                copy.start()

    def x_arrive(k):
        @pl.when(jnp.logical_not(forwards))
        def _():
            for copy in arrival(k, 3, x_recv):
                copy.wait_recv()

        @pl.when(jnp.logical_and(forwards, row > 0))
        def _():
            for copy in arrival(k, 1, b_recv):
                copy.wait_recv()

    def y_arrive(k):
        @pl.when(jnp.logical_and(row != 7, row != 2))
        def _():
            for copy in arrival(k, 3, y_recv):
                copy.wait_recv()

        @pl.when(row == 2)
        def _():
            for copy in arrival(k, 2, y_recv) + arrival(k, 1, c_recv):
                copy.wait_recv()

    flip = jnp.where(first, -1.0, 1.0)

    def radial(k):
        rows, lanes = piece(k)
        planes = [jnp.where(first, 4 - p, p) for p in (1, 2, 3)] + list(range(4, 11))
        stack = []
        for i, plane in enumerate(planes):
            cells = [column[c, plane, rows, lanes] for c in range(6)]
            if i < 3:
                cells[1] = cells[1] * flip
                cells[2] = cells[2] * flip
            inverse, pressure = primitives(cells, column_ph[plane, rows, lanes] == 1)
            stack.append((cells, cells[1] * inverse, pressure))
        for c in range(6):
            up, down = zip(*[split_flux(cells, v, p, 1, c) for cells, v, p in stack])

            def pieces(field):
                u = [field[i + 1] - field[i] for i in range(9)]
                d = [None] + [u[i] - u[i - 1] for i in range(1, 9)]
                q = [None] + [d[i] * d[i] + scaled_epsilon for i in range(1, 9)]
                return u, d, q

            u, d, q = pieces(up)
            right = [
                up[i] + correction(u[i - 2], u[i - 1], u[i], u[i + 1], d[i - 1], d[i], d[i + 1], q[i - 1], q[i], q[i + 1])
                for i in range(2, 7)
            ]
            u, d, q = pieces(down)
            left = [
                down[i] - correction(u[i + 1], u[i], u[i - 1], u[i - 2], -d[i + 1], -d[i], -d[i - 1], q[i + 1], q[i], q[i - 1])
                for i in range(3, 8)
            ]
            face = [a + b for a, b in zip(right, left)]
            weighted = [(row * 4 + j).astype(jnp.float32) * face[j] for j in range(5)]
            for j in range(4):
                radius = (row * 4 + j).astype(jnp.float32) + 0.5
                result[c, j, rows, lanes] = result[c, j, rows, lanes] - (weighted[j + 1] - weighted[j]) * (0.5 * quarter / radius)

    def axial_step(n, _):
        axial(n)
        return 0

    def azimuthal_steps(n, _):
        lax.fori_loop(2 * n, 2 * n + 2, azimuthal, 0)
        arrive_and_forward(n)
        return 0

    lax.fori_loop(0, 4, azimuthal_steps, 0)
    hand_over()
    for copy in z_copies():
        copy.wait_recv()

    def axial_steps(n, _):
        lax.fori_loop(2 * n, 2 * n + 2, axial_step, 0)

        @pl.when(n < 3)
        def _():
            arrive_and_forward(4 + n)

        return 0

    lax.fori_loop(0, 4, axial_steps, 0)

    @pl.when(row > 0)
    def _():
        arrive_and_forward(7)

    @pl.when(last)
    def _():
        for copy in rims():
            copy.wait()

    def tile(o):
        return pl.ds(o * 8, 8) if isinstance(o, int) else pl.ds(pl.multiple_of(o * 8, 8), 8)

    def out_copy(o):
        return pltpu.make_async_copy(result.at[:, :, tile(o), :], out_hbm.at[:, :, tile(o), :], out_sem.at[o])

    mine = pl.multiple_of(lax.rem(theta, 2) * 96, 8)
    other = pl.multiple_of(96 - lax.rem(theta, 2) * 96, 8)

    def share(step, o, source, target, where):
        return pltpu.make_async_remote_copy(
            src_ref=source,
            dst_ref=target,
            send_sem=f_send.at[4 * step + o],
            recv_sem=f_recv.at[4 * step + o],
            device_id={"theta": where},
            device_id_type=MESH,
        )

    def step_one(o):
        return share(0, o, part.at[o, pl.ds(other, 96)], half_got.at[o], sibling)

    def step_two(o):
        return share(1, o, half_sum.at[o], half_far.at[o], theta_far)

    def step_three(o):
        return share(2, o, half_total.at[o], half_peer.at[o], sibling)

    def filter_one(o):
        values = result[:, :, tile(o), :].reshape(192, 256)
        part[o] = product(values, table, table_low)
        step_one(o).start()

    def filter_two(o):
        step_one(o).wait_recv()
        half_sum[o] = part[o, pl.ds(mine, 96)] + half_got[o]
        step_two(o).start()

    def filter_three(o):
        step_two(o).wait_recv()
        half_total[o] = half_sum[o] + half_far[o]
        step_three(o).start()

    def filter_last(o, _):
        order = lax.broadcasted_iota(jnp.int32, (8, 128), 1)
        order = jnp.where(order < KMODES, order, order - KMODES)
        mode_scale = jnp.where(order == 0, 1.0 / NT, 2.0 / NT)
        weights = [jnp.where(order <= cutoff_smem[i], mode_scale, 0.0) for i in range(4)]
        weights = jnp.concatenate(weights * 3, 0)
        even_core = lax.rem(theta, 2) == 0
        step_three(o).wait_recv()
        own = half_total[o] * weights
        peer = half_peer[o] * weights
        lower = jnp.where(even_core, own, peer)
        upper = jnp.where(even_core, peer, own)
        coefficients = jnp.concatenate([lower, upper], 0)
        values = product(coefficients, table_t, table_t_low)
        result[:, :, tile(o), :] = values.reshape(6, 4, 8, 256)
        out_copy(o).start()
        return 0

    @pl.when(first)
    def _():
        for copy in table_loads():
            copy.wait()

    def radial_step(k, _):
        @pl.when(jnp.logical_and(first, k == 4))
        def _():
            arrive_and_forward(7)

        x_arrive(k)
        y_arrive(k)
        radial(k)
        o = k // 2
        whole = lax.rem(k, 2) == 1

        @pl.when(jnp.logical_and(whole, first))
        def _():
            filter_one(o)

            @pl.when(o > 0)
            def _():
                filter_two(o - 1)

        @pl.when(jnp.logical_and(whole, jnp.logical_not(first)))
        def _():
            out_copy(o).start()

        return 0

    lax.fori_loop(0, 8, radial_step, 0)

    @pl.when(first)
    def _():
        filter_two(3)
        for o in range(3):
            filter_three(o)
        lax.fori_loop(0, 3, filter_last, 0)
        filter_three(3)
        lax.fori_loop(3, 4, filter_last, 0)
        for o in range(4):
            step_one(o).wait_send()
            step_two(o).wait_send()
            step_three(o).wait_send()

    for copy in t_copies():
        copy.wait_send()
    for copy in z_copies():
        copy.wait_send()
    for k in range(8):
        for copy in x_first(k):
            copy.wait_send()

        @pl.when(inner_row)
        def _():
            for copy in x_fourth(k):
                copy.wait_send()

        @pl.when(first)
        def _():
            for copy in mirror(k) + forward_two(k):
                copy.wait_send()

        @pl.when(jnp.logical_and(forwards, row > 0))
        def _():
            for copy in forward(k):
                copy.wait_send()

    @pl.when(row == 1)
    def _():
        for k in range(DIRECT, 8):
            for copy in relay_on(k):
                copy.wait_send()

    @pl.when(row == 3)
    def _():
        for k in range(8):
            for copy in fourth_on(k):
                copy.wait_send()

    for o in range(4):
        out_copy(o).wait()


def fourier_tables():
    phases = (np.arange(NT)[:, None] * np.arange(KMODES)[None, :]) % NT
    angles = phases.astype(np.float64) * (2.0 * np.pi / NT)
    table = np.concatenate([np.cos(angles), np.sin(angles)], 1).astype(np.float32).reshape(4, 256, 2 * KMODES)
    halves = []
    for matrix in (table, np.ascontiguousarray(table.transpose(0, 2, 1))):
        high = matrix.astype(jnp.bfloat16)
        halves += [high, (matrix - high.astype(np.float32)).astype(jnp.bfloat16)]
    return halves


def shards(state_start, state_section, phase, cutoff):
    f32, i32 = jnp.float32, jnp.int32
    tables = [jnp.asarray(matrix) for matrix in fourier_tables()]
    anywhere = pl.BlockSpec(memory_space=pltpu.HBM)
    dma = pltpu.SemaphoreType.DMA
    return pl.pallas_call(
        kernel,
        out_shape=jax.ShapeDtypeStruct(state_start.shape, f32),
        in_specs=[anywhere] * 8,
        out_specs=anywhere,
        scratch_shapes=[
            pltpu.VMEM((6, 12, 32, 256), f32),
            pltpu.VMEM((12, 32, 256), i32),
            pltpu.VMEM((6, 4, 32, 256), f32),
            pltpu.VMEM((6, 4, 8, 256), f32),
            pltpu.VMEM((4, 8, 256), i32),
            pltpu.VMEM((6, 4, 8, 256), f32),
            pltpu.VMEM((4, 8, 256), i32),
            pltpu.VMEM((32, 128), f32),
            pltpu.VMEM((32, 128), f32),
            pltpu.VMEM((32, 128), f32),
            pltpu.VMEM((32, 128), f32),
            pltpu.VMEM((256, 2 * KMODES), jnp.bfloat16),
            pltpu.VMEM((256, 2 * KMODES), jnp.bfloat16),
            pltpu.VMEM((2 * KMODES, 256), jnp.bfloat16),
            pltpu.VMEM((2 * KMODES, 256), jnp.bfloat16),
            pltpu.VMEM((4, 192, 2 * KMODES), f32),
            pltpu.VMEM((4, 96, 2 * KMODES), f32),
            pltpu.VMEM((4, 96, 2 * KMODES), f32),
            pltpu.VMEM((4, 96, 2 * KMODES), f32),
            pltpu.VMEM((4, 96, 2 * KMODES), f32),
            pltpu.VMEM((4, 96, 2 * KMODES), f32),
            pltpu.VMEM((6, 3, 32, 256), f32),
            pltpu.VMEM((3, 32, 256), i32),
            pltpu.SMEM((4,), i32),
            dma((8,)),
            dma((8,)),
            dma((6,)),
            dma((6,)),
            *[dma((16,))] * 10,
            dma((4,)),
            dma((4,)),
            dma((2,)),
            dma((2,)),
            dma((12,)),
            dma((12,)),
            dma((4,)),
        ],
        compiler_params=pltpu.CompilerParams(collective_id=0, has_side_effects=True, vmem_limit_bytes=67043328),
        name="jet_section",
    )(state_start, state_section, phase, cutoff, *tables)


def solution(mesh):
    in_specs = (
        P(None, "row", "gz", "theta"),
        P(None, "row", "gz", "theta"),
        P("row", "gz", "theta"),
        P(),
    )
    out_specs = P(None, "row", "gz", "theta")
    return jax.shard_map(shards, mesh=mesh, in_specs=in_specs, out_specs=out_specs, check_vma=False)
```

```python
import functools
import math

import jax
import jax.numpy as jnp
import numpy as np
from jax import lax
from jax.experimental import pallas as pl
from jax.experimental.pallas import tpu as pltpu
from jax.sharding import PartitionSpec as P

NT = 1024
KMODES = 64
DIRECT = 3
ASIDE = 3

split_speed = 10.0
time_step = 0.05
weno_epsilon = 1e-06
scaled_epsilon = 4.0 * weno_epsilon * 12.0 / 13.0
side_scale = 3.0 / 13.0

MESH = pl.DeviceIdType.MESH


def primitives(cells, liquid):
    inverse = 1.0 / cells[0]
    kinetic = 0.5 * (cells[1] * cells[1] + cells[2] * cells[2] + cells[3] * cells[3]) * inverse
    internal = cells[4] - kinetic
    pressure = jnp.where(liquid, 3.4 * internal - 4.4 * 0.6, 0.4 * internal)
    return inverse, pressure


def split_flux(cells, velocity, pressure, component, channel):
    flux = cells[channel] * velocity
    if channel == component:
        flux = flux + pressure
    if channel == 4:
        flux = flux + pressure * velocity
    carried = split_speed * cells[channel]
    return flux + carried, flux - carried


def correction(u1, u2, u3, u4, d0, d1, d2, q0, q1, q2):
    a3 = 3.0 * u2
    b3 = 3.0 * u3
    g0 = a3 - u1
    g1 = u2 + u3
    g2 = u4 - b3
    t0 = q0 + (side_scale * g0) * g0
    t1 = q1 + (side_scale * g1) * g1
    t2 = q2 + (side_scale * g2) * g2
    s0 = t0 * t0
    s1 = t1 * t1
    s2 = t2 * t2
    p0 = s1 * s2
    p1 = (6.0 * s0) * s2
    p2 = (3.0 * s0) * s1
    z0 = d0 + d0 + a3
    z1 = g1 + u3
    z2 = b3 - d2
    top = p0 * z0 + p1 * z1 + p2 * z2
    bottom = p0 + p1 + p2
    return (top / bottom) * (1.0 / 6.0)


def line_divergence(upward, downward, axis):
    length = upward.shape[axis]

    def ahead(x, steps):
        return pltpu.roll(x, (-steps) % length, axis)

    def pieces(field):
        u = ahead(field, 1) - field
        um1 = ahead(u, -1)
        um2 = ahead(u, -2)
        up1 = ahead(u, 1)
        d1 = u - um1
        d0 = um1 - um2
        d2 = up1 - u
        return u, um1, um2, up1, d0, d1, d2, d0 * d0 + scaled_epsilon, d1 * d1 + scaled_epsilon, d2 * d2 + scaled_epsilon

    u, um1, um2, up1, d0, d1, d2, q0, q1, q2 = pieces(upward)
    right = upward + correction(um2, um1, u, up1, d0, d1, d2, q0, q1, q2)
    u, um1, um2, up1, d0, d1, d2, q0, q1, q2 = pieces(downward)
    left = downward - correction(up1, u, um1, um2, -d2, -d1, -d0, q2, q1, q0)
    face = right + ahead(left, 1)
    return face - ahead(face, -1)


def product(values, high_ref, low_ref):
    high = values.astype(jnp.bfloat16)
    low = (values - high.astype(jnp.float32)).astype(jnp.bfloat16)
    dot = functools.partial(jnp.dot, preferred_element_type=jnp.float32)
    return dot(high, high_ref[...]) + (dot(low, high_ref[...]) + dot(high, low_ref[...]))


def kernel(
    start_hbm,
    section_hbm,
    phase_hbm,
    cutoff_hbm,
    table_hbm,
    table_low_hbm,
    table_t_hbm,
    table_t_low_hbm,
    out_hbm,
    column,
    column_ph,
    result,
    z_low,
    z_low_ph,
    z_high,
    z_high_ph,
    pack_low,
    pack_high,
    got_low,
    got_high,
    table,
    table_low,
    table_t,
    table_t_low,
    part,
    half_got,
    half_sum,
    half_far,
    half_total,
    half_peer,
    relay,
    relay_ph,
    cutoff_smem,
    load_sem,
    load_ph_sem,
    rim_sem,
    misc_sem,
    x_send,
    x_recv,
    b_send,
    b_recv,
    y_send,
    y_recv,
    c_recv,
    m_send,
    r_send,
    r_recv,
    z_send,
    z_recv,
    t_send,
    t_recv,
    f_send,
    f_recv,
    out_sem,
):
    row = lax.axis_index("row")
    theta = lax.axis_index("theta")
    gz = lax.axis_index("gz")
    odd = lax.rem(row, 2)
    partner = row + 1 - 2 * odd
    theta_up = lax.rem(theta + 1, 4)
    theta_down = lax.rem(theta + 3, 4)
    theta_far = lax.rem(theta + 2, 4)
    sibling = theta + 1 - 2 * lax.rem(theta, 2)
    gz_up = lax.rem(gz + 1, 8)
    gz_down = lax.rem(gz + 7, 8)
    first = row == 0
    last = row == 7

    def piece(k):
        octet = k // 2
        half = k % 2
        if isinstance(k, int):
            return pl.ds(octet * 8, 8), pl.ds(half * 128, 128)
        return pl.ds(pl.multiple_of(octet * 8, 8), 8), pl.ds(pl.multiple_of(half * 128, 128), 128)

    def load(k):
        rows, lanes = piece(k)
        return (
            pltpu.make_async_copy(section_hbm.at[:, :, rows, lanes], column.at[:, pl.ds(4, 4), rows, lanes], load_sem.at[k]),
            pltpu.make_async_copy(phase_hbm.at[:, rows, lanes], column_ph.at[pl.ds(4, 4), rows, lanes], load_ph_sem.at[k]),
        )

    for k in range(8):
        for copy in load(k):
            copy.start()
    start_copy = pltpu.make_async_copy(start_hbm, result, misc_sem.at[0])
    start_copy.start()

    def rims():
        copies = []
        for j in range(3):
            copies.append(pltpu.make_async_copy(section_hbm.at[:, pl.ds(3, 1)], column.at[:, pl.ds(8 + j, 1)], rim_sem.at[2 * j]))
            copies.append(pltpu.make_async_copy(phase_hbm.at[pl.ds(3, 1)], column_ph.at[pl.ds(8 + j, 1)], rim_sem.at[2 * j + 1]))
        return copies

    def table_loads():
        return (
            pltpu.make_async_copy(table_hbm.at[theta], table, misc_sem.at[1]),
            pltpu.make_async_copy(table_t_hbm.at[theta], table_t, misc_sem.at[2]),
            pltpu.make_async_copy(table_low_hbm.at[theta], table_low, misc_sem.at[4]),
            pltpu.make_async_copy(table_t_low_hbm.at[theta], table_t_low, misc_sem.at[5]),
            pltpu.make_async_copy(cutoff_hbm, cutoff_smem, misc_sem.at[3]),
        )

    @pl.when(last)
    def _():
        for copy in rims():
            copy.start()

    @pl.when(first)
    def _():
        for copy in table_loads():
            copy.start()

    barrier = pltpu.get_barrier_semaphore()
    for where in (
        {"row": partner},
        {"row": lax.rem(row + 2, 8)},
        {"row": lax.rem(row + 6, 8)},
        {"theta": theta_up},
        {"theta": theta_down},
        {"theta": theta_far},
        {"row": partner, "theta": theta_far},
        {"gz": gz_up},
        {"gz": gz_down},
    ):
        pl.semaphore_signal(barrier, inc=1, device_id=where, device_id_type=MESH)

    def carry(k, source, target, count, send, recv, where):
        rows, lanes = piece(k)
        return (
            pltpu.make_async_remote_copy(
                src_ref=column.at[:, pl.ds(source, count), rows, lanes],
                dst_ref=column.at[:, pl.ds(target, count), rows, lanes],
                send_sem=send.at[k],
                recv_sem=recv.at[k],
                device_id=where,
                device_id_type=MESH,
            ),
            pltpu.make_async_remote_copy(
                src_ref=column_ph.at[pl.ds(source, count), rows, lanes],
                dst_ref=column_ph.at[pl.ds(target, count), rows, lanes],
                send_sem=send.at[k + 8],
                recv_sem=recv.at[k + 8],
                device_id=where,
                device_id_type=MESH,
            ),
        )

    for k in range(8):
        for copy in load(k):
            copy.wait()

    lane = lax.broadcasted_iota(jnp.int32, (8, 128), 1)

    def pack(n, _):
        rows = pl.ds(pl.multiple_of(n * 8, 8), 8)
        low = jnp.zeros((8, 128), jnp.float32)
        high = jnp.zeros((8, 128), jnp.float32)
        for group in range(28):
            channel, cycle = group % 7, 4 + group // 7
            if channel < 6:
                near = column[channel, cycle, rows, pl.ds(0, 128)]
                far = column[channel, cycle, rows, pl.ds(128, 128)]
            else:
                near = column_ph[cycle, rows, pl.ds(0, 128)].astype(jnp.float32)
                far = column_ph[cycle, rows, pl.ds(128, 128)].astype(jnp.float32)
            if group:
                near = pltpu.roll(near, 4 * group, 1)
            far = pltpu.roll(far, (4 * group + 4) % 128, 1)
            here = lane // 4 == group
            low = jnp.where(here, near, low)
            high = jnp.where(here, far, high)
        pack_low[rows, :] = low
        pack_high[rows, :] = high
        return 0

    lax.fori_loop(0, 4, pack, 0)

    inner_row = jnp.logical_and(row > 0, row < 7)
    to_partner = {"row": partner}

    swapped = jnp.logical_and(odd == 1, inner_row) & (row > 1)

    def x_three(k):
        return carry(k, jnp.where(swapped, 5, 4), jnp.where(swapped, 9, 8 * odd), 3, x_send, x_recv, to_partner)

    def x_fourth(k):
        return carry(k, jnp.where(swapped, 4, 7), jnp.where(swapped, 8, 3 + 8 * odd), 1, b_send, b_recv, to_partner)

    def x_first(k):
        return carry(k, 5, 1, 3, x_send, x_recv, to_partner)

    def mirror(k):
        return carry(k, 4, 1, 3, m_send, y_recv, {"theta": theta_far})

    def forward(k):
        target = jnp.where(odd == 1, lax.rem(row + 6, 8), lax.rem(row + 2, 8))
        return carry(k, 9 - 9 * odd, 1 + 7 * odd, 3, y_send, y_recv, {"row": target})

    def forward_two(k):
        return carry(k, 9, 1, 2, y_send, y_recv, {"row": 2})

    def forward_fourth(k):
        return carry(k, 11, 3, 1, b_send, c_recv, {"row": 2})

    def arrival(k, count, recv):
        return carry(k, 4, 4, count, x_send, recv, to_partner)

    def through(k, source, source_ph, target, target_ph, send, recv, where):
        rows, lanes = piece(k)
        return (
            pltpu.make_async_remote_copy(
                src_ref=source.at[:, :, rows, lanes],
                dst_ref=target.at[:, :, rows, lanes],
                send_sem=send.at[k],
                recv_sem=recv.at[k],
                device_id=where,
                device_id_type=MESH,
            ),
            pltpu.make_async_remote_copy(
                src_ref=source_ph.at[:, rows, lanes],
                dst_ref=target_ph.at[:, rows, lanes],
                send_sem=send.at[k + 8],
                recv_sem=recv.at[k + 8],
                device_id=where,
                device_id_type=MESH,
            ),
        )

    def planes_of(start, count):
        return column.at[:, pl.ds(start, count)], column_ph.at[pl.ds(start, count)]

    one_plane = relay.at[:, pl.ds(0, 1)], relay_ph.at[pl.ds(0, 1)]

    def relay_out(k):
        return through(k, *planes_of(5, 3), relay, relay_ph, x_send, r_recv, {"row": partner, "theta": theta_far})

    def relay_on(k):
        return through(k, relay, relay_ph, *planes_of(1, 3), r_send, x_recv, {"theta": theta_far})

    def fourth_out(k):
        return through(k, *planes_of(7, 1), *one_plane, b_send, r_recv, {"row": 3})

    def fourth_on(k):
        return through(k, *one_plane, *planes_of(3, 1), r_send, c_recv, {"row": 2})

    def hand_over():
        @pl.when(row == 1)
        def _():
            for k in range(DIRECT, 8):
                for copy in relay_out(k):
                    copy.wait_recv()
                for copy in relay_on(k):
                    copy.start()

        @pl.when(row == 3)
        def _():
            for k in range(ASIDE, 8):
                for copy in fourth_out(k):
                    copy.wait_recv()
                for copy in fourth_on(k):
                    copy.start()

    forwards = jnp.logical_or(jnp.logical_and(odd == 0, row < 6), jnp.logical_and(odd == 1, row > 1))

    def z_copies():
        copies = []
        for side, (rows, cells_to, phase_to, where) in enumerate(
            (
                (pl.ds(0, 8), z_high, z_high_ph, {"gz": gz_down}),
                (pl.ds(24, 8), z_low, z_low_ph, {"gz": gz_up}),
            )
        ):
            copies.append(
                pltpu.make_async_remote_copy(
                    src_ref=column.at[:, pl.ds(4, 4), rows, :],
                    dst_ref=cells_to,
                    send_sem=z_send.at[2 * side],
                    recv_sem=z_recv.at[2 * side],
                    device_id=where,
                    device_id_type=MESH,
                )
            )
            copies.append(
                pltpu.make_async_remote_copy(
                    src_ref=column_ph.at[pl.ds(4, 4), rows, :],
                    dst_ref=phase_to,
                    send_sem=z_send.at[2 * side + 1],
                    recv_sem=z_recv.at[2 * side + 1],
                    device_id=where,
                    device_id_type=MESH,
                )
            )
        return copies

    def t_copies():
        return (
            pltpu.make_async_remote_copy(
                src_ref=pack_low,
                dst_ref=got_high,
                send_sem=t_send.at[0],
                recv_sem=t_recv.at[0],
                device_id={"theta": theta_down},
                device_id_type=MESH,
            ),
            pltpu.make_async_remote_copy(
                src_ref=pack_high,
                dst_ref=got_low,
                send_sem=t_send.at[1],
                recv_sem=t_recv.at[1],
                device_id={"theta": theta_up},
                device_id_type=MESH,
            ),
        )

    pl.semaphore_wait(barrier, 9)
    for copy in t_copies():
        copy.start()
    for copy in z_copies():
        copy.start()

    @pl.when(inner_row)
    def _():
        for k in range(8):
            for copy in x_three(k):
                copy.start()

        @pl.when(row > 1)
        def _():
            for k in range(8):
                for copy in x_fourth(k):
                    copy.start()

        @pl.when(row == 1)
        def _():
            for k in range(ASIDE):
                for copy in x_fourth(k):
                    copy.start()
            for k in range(ASIDE, 8):
                for copy in fourth_out(k):
                    copy.start()

    @pl.when(first)
    def _():
        for k in range(8):
            for copy in mirror(k):
                copy.start()
            if k >= DIRECT:
                for copy in relay_out(k):
                    copy.start()
        for k in range(DIRECT):
            for copy in x_first(k):
                copy.start()

    @pl.when(last)
    def _():
        for k in range(8):
            for copy in x_three(k):
                copy.start()

    start_copy.wait()
    for copy in t_copies():
        copy.wait_recv()

    quarter = 0.25 * time_step

    lane16 = lax.broadcasted_iota(jnp.int32, (16, 128), 1)

    def azimuthal(n, _):
        cycle = n // 2
        rows = pl.ds(pl.multiple_of((n % 2) * 16, 8), 16)
        low = got_low[rows, :]
        high = got_high[rows, :]
        base = cycle * 28

        def edge(channel):
            offset = base + 4 * channel
            upper = pltpu.roll(high, lax.rem(128 - offset, 128), 1)
            lower = pltpu.roll(low, 124 - offset, 1)
            return jnp.where(lane16 < 64, upper, lower)

        cells = [jnp.concatenate([column[c, 4 + cycle, rows, :], edge(c)], 1) for c in range(6)]
        old = [result[c, cycle, rows, :] for c in range(6)]
        new = []
        material = jnp.concatenate([column_ph[4 + cycle, rows, :].astype(jnp.float32), edge(6)], 1)
        inverse, pressure = primitives(cells, material > 0.5)
        velocity = cells[2] * inverse
        radius = (row * 4 + cycle).astype(jnp.float32) + 0.5
        scale = 0.5 * quarter / (radius * (2.0 * math.pi / NT))
        source_scale = quarter / radius
        for c in range(6):
            upward, downward = split_flux(cells, velocity, pressure, 2, c)
            change = line_divergence(upward, downward, 1)[:, :256] * scale
            value = 0.75 * old[c] + 0.25 * cells[c][:, :256] - change
            if c == 1:
                value = value + source_scale * (cells[2] * velocity + pressure)[:, :256]
            if c == 2:
                value = value - source_scale * (cells[1] * velocity)[:, :256]
            new.append(value)
        for c in range(6):
            result[c, cycle, rows, :] = new[c]
        return 0

    row8 = lax.broadcasted_iota(jnp.int32, (8, 128), 0)

    def axial(n):
        cycle = n // 2
        lanes = pl.ds(pl.multiple_of((n % 2) * 128, 128), 128)
        cells = [
            jnp.concatenate(
                [column[c, 4 + cycle, :, lanes], jnp.where(row8 < 4, z_high[c, cycle, :, lanes], z_low[c, cycle, :, lanes])], 0
            )
            for c in range(6)
        ]
        material = jnp.concatenate(
            [column_ph[4 + cycle, :, lanes], jnp.where(row8 < 4, z_high_ph[cycle, :, lanes], z_low_ph[cycle, :, lanes])], 0
        )
        inverse, pressure = primitives(cells, material == 1)
        velocity = cells[3] * inverse
        for c in range(6):
            upward, downward = split_flux(cells, velocity, pressure, 3, c)
            change = line_divergence(upward, downward, 0)[:32] * (0.5 * quarter)
            result[c, cycle, :, lanes] = result[c, cycle, :, lanes] - change

    def arrive_and_forward(k):
        @pl.when(forwards)
        def _():
            for copy in arrival(k, 3, x_recv):
                copy.wait_recv()

        @pl.when(jnp.logical_and(forwards, row > 0))
        def _():
            for copy in forward(k):
                copy.start()

        @pl.when(first)
        def _():
            for copy in forward_two(k):
                copy.start()

    def x_arrive(k):
        @pl.when(jnp.logical_not(forwards))
        def _():
            for copy in arrival(k, 3, x_recv):
                copy.wait_recv()

        @pl.when(jnp.logical_and(forwards, row > 0))
        def _():
            for copy in arrival(k, 1, b_recv):
                copy.wait_recv()

    def y_arrive(k):
        @pl.when(jnp.logical_and(row != 7, row != 2))
        def _():
            for copy in arrival(k, 3, y_recv):
                copy.wait_recv()

        @pl.when(row == 2)
        def _():
            for copy in arrival(k, 2, y_recv) + arrival(k, 1, c_recv):
                copy.wait_recv()

    flip = jnp.where(first, -1.0, 1.0)

    def radial(k):
        rows, lanes = piece(k)
        planes = [jnp.where(first, 4 - p, p) for p in (1, 2, 3)] + list(range(4, 11))
        stack = []
        for i, plane in enumerate(planes):
            cells = [column[c, plane, rows, lanes] for c in range(6)]
            if i < 3:
                cells[1] = cells[1] * flip
                cells[2] = cells[2] * flip
            inverse, pressure = primitives(cells, column_ph[plane, rows, lanes] == 1)
            stack.append((cells, cells[1] * inverse, pressure))
        for c in range(6):
            up, down = zip(*[split_flux(cells, v, p, 1, c) for cells, v, p in stack])

            def pieces(field):
                u = [field[i + 1] - field[i] for i in range(9)]
                d = [None] + [u[i] - u[i - 1] for i in range(1, 9)]
                q = [None] + [d[i] * d[i] + scaled_epsilon for i in range(1, 9)]
                return u, d, q

            u, d, q = pieces(up)
            right = [
                up[i] + correction(u[i - 2], u[i - 1], u[i], u[i + 1], d[i - 1], d[i], d[i + 1], q[i - 1], q[i], q[i + 1])
                for i in range(2, 7)
            ]
            u, d, q = pieces(down)
            left = [
                down[i] - correction(u[i + 1], u[i], u[i - 1], u[i - 2], -d[i + 1], -d[i], -d[i - 1], q[i + 1], q[i], q[i - 1])
                for i in range(3, 8)
            ]
            face = [a + b for a, b in zip(right, left)]
            weighted = [(row * 4 + j).astype(jnp.float32) * face[j] for j in range(5)]
            for j in range(4):
                radius = (row * 4 + j).astype(jnp.float32) + 0.5
                result[c, j, rows, lanes] = result[c, j, rows, lanes] - (weighted[j + 1] - weighted[j]) * (0.5 * quarter / radius)

    def axial_step(n, _):
        axial(n)
        return 0

    def azimuthal_steps(n, _):
        lax.fori_loop(2 * n, 2 * n + 2, azimuthal, 0)
        arrive_and_forward(n)
        return 0

    lax.fori_loop(0, 4, azimuthal_steps, 0)
    hand_over()
    for copy in z_copies():
        copy.wait_recv()

    def axial_steps(n, _):
        lax.fori_loop(2 * n, 2 * n + 2, axial_step, 0)

        @pl.when(jnp.logical_and(row > 0, n < 3))
        def _():
            arrive_and_forward(4 + n)

        return 0

    lax.fori_loop(0, 4, axial_steps, 0)

    @pl.when(row > 0)
    def _():
        arrive_and_forward(7)

    @pl.when(first)
    def _():
        arrive_and_forward(4)
        arrive_and_forward(5)

    @pl.when(last)
    def _():
        for copy in rims():
            copy.wait()

    def tile(o):
        return pl.ds(o * 8, 8) if isinstance(o, int) else pl.ds(pl.multiple_of(o * 8, 8), 8)

    def out_copy(o):
        return pltpu.make_async_copy(result.at[:, :, tile(o), :], out_hbm.at[:, :, tile(o), :], out_sem.at[o])

    mine = pl.multiple_of(lax.rem(theta, 2) * 96, 8)
    other = pl.multiple_of(96 - lax.rem(theta, 2) * 96, 8)

    def share(step, o, source, target, where):
        return pltpu.make_async_remote_copy(
            src_ref=source,
            dst_ref=target,
            send_sem=f_send.at[4 * step + o],
            recv_sem=f_recv.at[4 * step + o],
            device_id={"theta": where},
            device_id_type=MESH,
        )

    def step_one(o):
        return share(0, o, part.at[o, pl.ds(other, 96)], half_got.at[o], sibling)

    def step_two(o):
        return share(1, o, half_sum.at[o], half_far.at[o], theta_far)

    def step_three(o):
        return share(2, o, half_total.at[o], half_peer.at[o], sibling)

    def filter_one(o):
        values = result[:, :, tile(o), :].reshape(192, 256)
        part[o] = product(values, table, table_low)
        step_one(o).start()

    def filter_two(o):
        step_one(o).wait_recv()
        half_sum[o] = part[o, pl.ds(mine, 96)] + half_got[o]
        step_two(o).start()

    def filter_three(o):
        step_two(o).wait_recv()
        half_total[o] = half_sum[o] + half_far[o]
        step_three(o).start()

    def filter_last(o, _):
        order = lax.broadcasted_iota(jnp.int32, (8, 128), 1)
        order = jnp.where(order < KMODES, order, order - KMODES)
        mode_scale = jnp.where(order == 0, 1.0 / NT, 2.0 / NT)
        weights = [jnp.where(order <= cutoff_smem[i], mode_scale, 0.0) for i in range(4)]
        weights = jnp.concatenate(weights * 3, 0)
        even_core = lax.rem(theta, 2) == 0
        step_three(o).wait_recv()
        own = half_total[o] * weights
        peer = half_peer[o] * weights
        lower = jnp.where(even_core, own, peer)
        upper = jnp.where(even_core, peer, own)
        coefficients = jnp.concatenate([lower, upper], 0)
        values = product(coefficients, table_t, table_t_low)
        result[:, :, tile(o), :] = values.reshape(6, 4, 8, 256)
        out_copy(o).start()
        return 0

    @pl.when(first)
    def _():
        for copy in table_loads():
            copy.wait()

    def radial_step(k, _):
        @pl.when(jnp.logical_and(first, k == 2))
        def _():
            arrive_and_forward(6)

        @pl.when(jnp.logical_and(first, k == 5))
        def _():
            arrive_and_forward(7)

        @pl.when(jnp.logical_and(first, jnp.logical_and(k > 4, k < 5 + ASIDE)))
        def _():
            for copy in arrival(k - 5, 1, b_recv):
                copy.wait_recv()
            for copy in forward_fourth(k - 5):
                copy.start()

        x_arrive(k)
        y_arrive(k)
        radial(k)
        o = k // 2
        whole = lax.rem(k, 2) == 1

        @pl.when(jnp.logical_and(whole, first))
        def _():
            filter_one(o)

            @pl.when(o > 0)
            def _():
                filter_two(o - 1)

        @pl.when(jnp.logical_and(whole, jnp.logical_not(first)))
        def _():
            out_copy(o).start()

        return 0

    lax.fori_loop(0, 8, radial_step, 0)

    @pl.when(first)
    def _():
        filter_two(3)
        for o in range(3):
            filter_three(o)
        lax.fori_loop(0, 2, filter_last, 0)
        filter_three(3)
        lax.fori_loop(2, 4, filter_last, 0)
        for k in range(ASIDE):
            for copy in forward_fourth(k):
                copy.wait_send()
        for o in range(4):
            step_one(o).wait_send()
            step_two(o).wait_send()
            step_three(o).wait_send()

    for copy in t_copies():
        copy.wait_send()
    for copy in z_copies():
        copy.wait_send()
    for k in range(8):
        for copy in x_first(k):
            copy.wait_send()

        @pl.when(inner_row)
        def _():
            for copy in x_fourth(k):
                copy.wait_send()

        @pl.when(first)
        def _():
            for copy in mirror(k) + forward_two(k):
                copy.wait_send()

        @pl.when(jnp.logical_and(forwards, row > 0))
        def _():
            for copy in forward(k):
                copy.wait_send()

    @pl.when(row == 1)
    def _():
        for k in range(DIRECT, 8):
            for copy in relay_on(k):
                copy.wait_send()

    @pl.when(row == 3)
    def _():
        for k in range(ASIDE, 8):
            for copy in fourth_on(k):
                copy.wait_send()

    for o in range(4):
        out_copy(o).wait()


def fourier_tables():
    phases = (np.arange(NT)[:, None] * np.arange(KMODES)[None, :]) % NT
    angles = phases.astype(np.float64) * (2.0 * np.pi / NT)
    table = np.concatenate([np.cos(angles), np.sin(angles)], 1).astype(np.float32).reshape(4, 256, 2 * KMODES)
    halves = []
    for matrix in (table, np.ascontiguousarray(table.transpose(0, 2, 1))):
        high = matrix.astype(jnp.bfloat16)
        halves += [high, (matrix - high.astype(np.float32)).astype(jnp.bfloat16)]
    return halves


def shards(state_start, state_section, phase, cutoff):
    f32, i32 = jnp.float32, jnp.int32
    tables = [jnp.asarray(matrix) for matrix in fourier_tables()]
    anywhere = pl.BlockSpec(memory_space=pltpu.HBM)
    dma = pltpu.SemaphoreType.DMA
    return pl.pallas_call(
        kernel,
        out_shape=jax.ShapeDtypeStruct(state_start.shape, f32),
        in_specs=[anywhere] * 8,
        out_specs=anywhere,
        scratch_shapes=[
            pltpu.VMEM((6, 12, 32, 256), f32),
            pltpu.VMEM((12, 32, 256), i32),
            pltpu.VMEM((6, 4, 32, 256), f32),
            pltpu.VMEM((6, 4, 8, 256), f32),
            pltpu.VMEM((4, 8, 256), i32),
            pltpu.VMEM((6, 4, 8, 256), f32),
            pltpu.VMEM((4, 8, 256), i32),
            pltpu.VMEM((32, 128), f32),
            pltpu.VMEM((32, 128), f32),
            pltpu.VMEM((32, 128), f32),
            pltpu.VMEM((32, 128), f32),
            pltpu.VMEM((256, 2 * KMODES), jnp.bfloat16),
            pltpu.VMEM((256, 2 * KMODES), jnp.bfloat16),
            pltpu.VMEM((2 * KMODES, 256), jnp.bfloat16),
            pltpu.VMEM((2 * KMODES, 256), jnp.bfloat16),
            pltpu.VMEM((4, 192, 2 * KMODES), f32),
            pltpu.VMEM((4, 96, 2 * KMODES), f32),
            pltpu.VMEM((4, 96, 2 * KMODES), f32),
            pltpu.VMEM((4, 96, 2 * KMODES), f32),
            pltpu.VMEM((4, 96, 2 * KMODES), f32),
            pltpu.VMEM((4, 96, 2 * KMODES), f32),
            pltpu.VMEM((6, 3, 32, 256), f32),
            pltpu.VMEM((3, 32, 256), i32),
            pltpu.SMEM((4,), i32),
            dma((8,)),
            dma((8,)),
            dma((6,)),
            dma((6,)),
            *[dma((16,))] * 10,
            dma((4,)),
            dma((4,)),
            dma((2,)),
            dma((2,)),
            dma((12,)),
            dma((12,)),
            dma((4,)),
        ],
        compiler_params=pltpu.CompilerParams(collective_id=0, has_side_effects=True, vmem_limit_bytes=67043328),
        name="jet_section",
    )(state_start, state_section, phase, cutoff, *tables)


def solution(mesh):
    in_specs = (
        P(None, "row", "gz", "theta"),
        P(None, "row", "gz", "theta"),
        P("row", "gz", "theta"),
        P(),
    )
    out_specs = P(None, "row", "gz", "theta")
    return jax.shard_map(shards, mesh=mesh, in_specs=in_specs, out_specs=out_specs, check_vma=False)
```

```python
import functools
import math

import jax
import jax.numpy as jnp
import numpy as np
from jax import lax
from jax.experimental import pallas as pl
from jax.experimental.pallas import tpu as pltpu
from jax.sharding import PartitionSpec as P

NT = 1024
KMODES = 64
DIRECT = 3
ASIDE = 3

split_speed = 10.0
time_step = 0.05
weno_epsilon = 1e-06
scaled_epsilon = 4.0 * weno_epsilon * 12.0 / 13.0
side_scale = 3.0 / 13.0

MESH = pl.DeviceIdType.MESH


def primitives(cells, liquid):
    inverse = 1.0 / cells[0]
    kinetic = 0.5 * (cells[1] * cells[1] + cells[2] * cells[2] + cells[3] * cells[3]) * inverse
    internal = cells[4] - kinetic
    pressure = jnp.where(liquid, 3.4 * internal - 4.4 * 0.6, 0.4 * internal)
    return inverse, pressure


def split_flux(cells, velocity, pressure, component, channel):
    flux = cells[channel] * velocity
    if channel == component:
        flux = flux + pressure
    if channel == 4:
        flux = flux + pressure * velocity
    carried = split_speed * cells[channel]
    return flux + carried, flux - carried


def correction(u1, u2, u3, u4, d0, d1, d2, q0, q1, q2):
    a3 = 3.0 * u2
    b3 = 3.0 * u3
    g0 = a3 - u1
    g1 = u2 + u3
    g2 = u4 - b3
    t0 = q0 + (side_scale * g0) * g0
    t1 = q1 + (side_scale * g1) * g1
    t2 = q2 + (side_scale * g2) * g2
    s0 = t0 * t0
    s1 = t1 * t1
    s2 = t2 * t2
    p0 = s1 * s2
    p1 = (6.0 * s0) * s2
    p2 = (3.0 * s0) * s1
    z0 = d0 + d0 + a3
    z1 = g1 + u3
    z2 = b3 - d2
    top = p0 * z0 + p1 * z1 + p2 * z2
    bottom = p0 + p1 + p2
    return (top / bottom) * (1.0 / 6.0)


def line_divergence(upward, downward, axis):
    length = upward.shape[axis]

    def ahead(x, steps):
        return pltpu.roll(x, (-steps) % length, axis)

    def pieces(field):
        u = ahead(field, 1) - field
        um1 = ahead(u, -1)
        um2 = ahead(u, -2)
        up1 = ahead(u, 1)
        d1 = u - um1
        d0 = um1 - um2
        d2 = up1 - u
        return u, um1, um2, up1, d0, d1, d2, d0 * d0 + scaled_epsilon, d1 * d1 + scaled_epsilon, d2 * d2 + scaled_epsilon

    u, um1, um2, up1, d0, d1, d2, q0, q1, q2 = pieces(upward)
    right = upward + correction(um2, um1, u, up1, d0, d1, d2, q0, q1, q2)
    u, um1, um2, up1, d0, d1, d2, q0, q1, q2 = pieces(downward)
    left = downward - correction(up1, u, um1, um2, -d2, -d1, -d0, q2, q1, q0)
    face = right + ahead(left, 1)
    return face - ahead(face, -1)


def product(values, high_ref, low_ref):
    high = values.astype(jnp.bfloat16)
    low = (values - high.astype(jnp.float32)).astype(jnp.bfloat16)
    dot = functools.partial(jnp.dot, preferred_element_type=jnp.float32)
    return dot(high, high_ref[...]) + (dot(low, high_ref[...]) + dot(high, low_ref[...]))


def kernel(
    start_hbm,
    section_hbm,
    phase_hbm,
    cutoff_hbm,
    table_hbm,
    table_low_hbm,
    table_t_hbm,
    table_t_low_hbm,
    out_hbm,
    column,
    column_ph,
    result,
    z_low,
    z_low_ph,
    z_high,
    z_high_ph,
    pack_low,
    pack_high,
    got_low,
    got_high,
    table,
    table_low,
    table_t,
    table_t_low,
    part,
    half_got,
    half_sum,
    half_far,
    half_total,
    half_peer,
    relay,
    relay_ph,
    cutoff_smem,
    load_sem,
    load_ph_sem,
    rim_sem,
    misc_sem,
    x_send,
    x_recv,
    b_send,
    b_recv,
    y_send,
    y_recv,
    c_recv,
    m_send,
    r_send,
    r_recv,
    z_send,
    z_recv,
    t_send,
    t_recv,
    f_send,
    f_recv,
    out_sem,
):
    row = lax.axis_index("row")
    theta = lax.axis_index("theta")
    gz = lax.axis_index("gz")
    odd = lax.rem(row, 2)
    partner = row + 1 - 2 * odd
    theta_up = lax.rem(theta + 1, 4)
    theta_down = lax.rem(theta + 3, 4)
    theta_far = lax.rem(theta + 2, 4)
    sibling = theta + 1 - 2 * lax.rem(theta, 2)
    gz_up = lax.rem(gz + 1, 8)
    gz_down = lax.rem(gz + 7, 8)
    first = row == 0
    last = row == 7

    def piece(k):
        octet = k // 2
        half = k % 2
        if isinstance(k, int):
            return pl.ds(octet * 8, 8), pl.ds(half * 128, 128)
        return pl.ds(pl.multiple_of(octet * 8, 8), 8), pl.ds(pl.multiple_of(half * 128, 128), 128)

    def load(k):
        rows, lanes = piece(k)
        return (
            pltpu.make_async_copy(section_hbm.at[:, :, rows, lanes], column.at[:, pl.ds(4, 4), rows, lanes], load_sem.at[k]),
            pltpu.make_async_copy(phase_hbm.at[:, rows, lanes], column_ph.at[pl.ds(4, 4), rows, lanes], load_ph_sem.at[k]),
        )

    for k in range(8):
        for copy in load(k):
            copy.start()
    start_copy = pltpu.make_async_copy(start_hbm, result, misc_sem.at[0])
    start_copy.start()

    def rims():
        copies = []
        for j in range(3):
            copies.append(pltpu.make_async_copy(section_hbm.at[:, pl.ds(3, 1)], column.at[:, pl.ds(8 + j, 1)], rim_sem.at[2 * j]))
            copies.append(pltpu.make_async_copy(phase_hbm.at[pl.ds(3, 1)], column_ph.at[pl.ds(8 + j, 1)], rim_sem.at[2 * j + 1]))
        return copies

    def table_loads():
        return (
            pltpu.make_async_copy(table_hbm.at[theta], table, misc_sem.at[1]),
            pltpu.make_async_copy(table_t_hbm.at[theta], table_t, misc_sem.at[2]),
            pltpu.make_async_copy(table_low_hbm.at[theta], table_low, misc_sem.at[4]),
            pltpu.make_async_copy(table_t_low_hbm.at[theta], table_t_low, misc_sem.at[5]),
            pltpu.make_async_copy(cutoff_hbm, cutoff_smem, misc_sem.at[3]),
        )

    @pl.when(last)
    def _():
        for copy in rims():
            copy.start()

    @pl.when(first)
    def _():
        for copy in table_loads():
            copy.start()

    barrier = pltpu.get_barrier_semaphore()
    for where in (
        {"row": partner},
        {"row": lax.rem(row + 2, 8)},
        {"row": lax.rem(row + 6, 8)},
        {"theta": theta_up},
        {"theta": theta_down},
        {"theta": theta_far},
        {"row": partner, "theta": theta_far},
        {"gz": gz_up},
        {"gz": gz_down},
    ):
        pl.semaphore_signal(barrier, inc=1, device_id=where, device_id_type=MESH)

    def carry(k, source, target, count, send, recv, where):
        rows, lanes = piece(k)
        return (
            pltpu.make_async_remote_copy(
                src_ref=column.at[:, pl.ds(source, count), rows, lanes],
                dst_ref=column.at[:, pl.ds(target, count), rows, lanes],
                send_sem=send.at[k],
                recv_sem=recv.at[k],
                device_id=where,
                device_id_type=MESH,
            ),
            pltpu.make_async_remote_copy(
                src_ref=column_ph.at[pl.ds(source, count), rows, lanes],
                dst_ref=column_ph.at[pl.ds(target, count), rows, lanes],
                send_sem=send.at[k + 8],
                recv_sem=recv.at[k + 8],
                device_id=where,
                device_id_type=MESH,
            ),
        )

    for k in range(8):
        for copy in load(k):
            copy.wait()

    lane = lax.broadcasted_iota(jnp.int32, (8, 128), 1)

    def pack(n, _):
        rows = pl.ds(pl.multiple_of(n * 8, 8), 8)
        low = jnp.zeros((8, 128), jnp.float32)
        high = jnp.zeros((8, 128), jnp.float32)
        for group in range(28):
            channel, cycle = group % 7, 4 + group // 7
            if channel < 6:
                near = column[channel, cycle, rows, pl.ds(0, 128)]
                far = column[channel, cycle, rows, pl.ds(128, 128)]
            else:
                near = column_ph[cycle, rows, pl.ds(0, 128)].astype(jnp.float32)
                far = column_ph[cycle, rows, pl.ds(128, 128)].astype(jnp.float32)
            if group:
                near = pltpu.roll(near, 4 * group, 1)
            far = pltpu.roll(far, (4 * group + 4) % 128, 1)
            here = lane // 4 == group
            low = jnp.where(here, near, low)
            high = jnp.where(here, far, high)
        pack_low[rows, :] = low
        pack_high[rows, :] = high
        return 0

    lax.fori_loop(0, 4, pack, 0)

    inner_row = jnp.logical_and(row > 0, row < 7)
    to_partner = {"row": partner}

    swapped = jnp.logical_and(odd == 1, inner_row) & (row > 1)

    def x_three(k):
        return carry(k, jnp.where(swapped, 5, 4), jnp.where(swapped, 9, 8 * odd), 3, x_send, x_recv, to_partner)

    def x_fourth(k):
        return carry(k, jnp.where(swapped, 4, 7), jnp.where(swapped, 8, 3 + 8 * odd), 1, b_send, b_recv, to_partner)

    def x_first(k):
        return carry(k, 5, 1, 3, x_send, x_recv, to_partner)

    def mirror(k):
        return carry(k, 4, 1, 3, m_send, y_recv, {"theta": theta_far})

    def forward(k):
        target = jnp.where(odd == 1, lax.rem(row + 6, 8), lax.rem(row + 2, 8))
        return carry(k, 9 - 9 * odd, 1 + 7 * odd, 3, y_send, y_recv, {"row": target})

    def forward_two(k):
        return carry(k, 9, 1, 2, y_send, y_recv, {"row": 2})

    def forward_fourth(k):
        return carry(k, 11, 3, 1, b_send, c_recv, {"row": 2})

    def arrival(k, count, recv):
        return carry(k, 4, 4, count, x_send, recv, to_partner)

    def through(k, source, source_ph, target, target_ph, send, recv, where):
        rows, lanes = piece(k)
        return (
            pltpu.make_async_remote_copy(
                src_ref=source.at[:, :, rows, lanes],
                dst_ref=target.at[:, :, rows, lanes],
                send_sem=send.at[k],
                recv_sem=recv.at[k],
                device_id=where,
                device_id_type=MESH,
            ),
            pltpu.make_async_remote_copy(
                src_ref=source_ph.at[:, rows, lanes],
                dst_ref=target_ph.at[:, rows, lanes],
                send_sem=send.at[k + 8],
                recv_sem=recv.at[k + 8],
                device_id=where,
                device_id_type=MESH,
            ),
        )

    def planes_of(start, count):
        return column.at[:, pl.ds(start, count)], column_ph.at[pl.ds(start, count)]

    one_plane = relay.at[:, pl.ds(0, 1)], relay_ph.at[pl.ds(0, 1)]

    def relay_out(k):
        return through(k, *planes_of(5, 3), relay, relay_ph, x_send, r_recv, {"row": partner, "theta": theta_far})

    def relay_on(k):
        return through(k, relay, relay_ph, *planes_of(1, 3), r_send, x_recv, {"theta": theta_far})

    def fourth_out(k):
        return through(k, *planes_of(7, 1), *one_plane, b_send, r_recv, {"row": 3})

    def fourth_on(k):
        return through(k, *one_plane, *planes_of(3, 1), r_send, c_recv, {"row": 2})

    def hand_over():
        @pl.when(row == 1)
        def _():
            for k in range(DIRECT, 8):
                for copy in relay_out(k):
                    copy.wait_recv()
                for copy in relay_on(k):
                    copy.start()

        @pl.when(row == 3)
        def _():
            for k in range(ASIDE, 8):
                for copy in fourth_out(k):
                    copy.wait_recv()
                for copy in fourth_on(k):
                    copy.start()

    forwards = jnp.logical_or(jnp.logical_and(odd == 0, row < 6), jnp.logical_and(odd == 1, row > 1))

    def z_copies():
        copies = []
        for side, (rows, cells_to, phase_to, where) in enumerate(
            (
                (pl.ds(0, 8), z_high, z_high_ph, {"gz": gz_down}),
                (pl.ds(24, 8), z_low, z_low_ph, {"gz": gz_up}),
            )
        ):
            copies.append(
                pltpu.make_async_remote_copy(
                    src_ref=column.at[:, pl.ds(4, 4), rows, :],
                    dst_ref=cells_to,
                    send_sem=z_send.at[2 * side],
                    recv_sem=z_recv.at[2 * side],
                    device_id=where,
                    device_id_type=MESH,
                )
            )
            copies.append(
                pltpu.make_async_remote_copy(
                    src_ref=column_ph.at[pl.ds(4, 4), rows, :],
                    dst_ref=phase_to,
                    send_sem=z_send.at[2 * side + 1],
                    recv_sem=z_recv.at[2 * side + 1],
                    device_id=where,
                    device_id_type=MESH,
                )
            )
        return copies

    def t_copies():
        return (
            pltpu.make_async_remote_copy(
                src_ref=pack_low,
                dst_ref=got_high,
                send_sem=t_send.at[0],
                recv_sem=t_recv.at[0],
                device_id={"theta": theta_down},
                device_id_type=MESH,
            ),
            pltpu.make_async_remote_copy(
                src_ref=pack_high,
                dst_ref=got_low,
                send_sem=t_send.at[1],
                recv_sem=t_recv.at[1],
                device_id={"theta": theta_up},
                device_id_type=MESH,
            ),
        )

    pl.semaphore_wait(barrier, 9)
    for copy in t_copies():
        copy.start()
    for copy in z_copies():
        copy.start()

    @pl.when(inner_row)
    def _():
        for k in range(8):
            for copy in x_three(k):
                copy.start()

        @pl.when(row > 1)
        def _():
            for k in range(8):
                for copy in x_fourth(k):
                    copy.start()

        @pl.when(row == 1)
        def _():
            for k in range(ASIDE):
                for copy in x_fourth(k):
                    copy.start()
            for k in range(ASIDE, 8):
                for copy in fourth_out(k):
                    copy.start()

    @pl.when(first)
    def _():
        for k in range(8):
            for copy in mirror(k):
                copy.start()
            if k >= DIRECT:
                for copy in relay_out(k):
                    copy.start()
        for k in range(DIRECT):
            for copy in x_first(k):
                copy.start()

    @pl.when(last)
    def _():
        for k in range(8):
            for copy in x_three(k):
                copy.start()

    start_copy.wait()
    for copy in t_copies():
        copy.wait_recv()

    quarter = 0.25 * time_step

    lane16 = lax.broadcasted_iota(jnp.int32, (16, 128), 1)

    def azimuthal(n, _):
        cycle = n // 2
        rows = pl.ds(pl.multiple_of((n % 2) * 16, 8), 16)
        low = got_low[rows, :]
        high = got_high[rows, :]
        base = cycle * 28

        def edge(channel):
            offset = base + 4 * channel
            upper = pltpu.roll(high, lax.rem(128 - offset, 128), 1)
            lower = pltpu.roll(low, 124 - offset, 1)
            return jnp.where(lane16 < 64, upper, lower)

        cells = [jnp.concatenate([column[c, 4 + cycle, rows, :], edge(c)], 1) for c in range(6)]
        old = [result[c, cycle, rows, :] for c in range(6)]
        new = []
        material = jnp.concatenate([column_ph[4 + cycle, rows, :].astype(jnp.float32), edge(6)], 1)
        inverse, pressure = primitives(cells, material > 0.5)
        velocity = cells[2] * inverse
        radius = (row * 4 + cycle).astype(jnp.float32) + 0.5
        scale = 0.5 * quarter / (radius * (2.0 * math.pi / NT))
        source_scale = quarter / radius
        for c in range(6):
            upward, downward = split_flux(cells, velocity, pressure, 2, c)
            change = line_divergence(upward, downward, 1)[:, :256] * scale
            value = 0.75 * old[c] + 0.25 * cells[c][:, :256] - change
            if c == 1:
                value = value + source_scale * (cells[2] * velocity + pressure)[:, :256]
            if c == 2:
                value = value - source_scale * (cells[1] * velocity)[:, :256]
            new.append(value)
        for c in range(6):
            result[c, cycle, rows, :] = new[c]
        return 0

    row8 = lax.broadcasted_iota(jnp.int32, (8, 128), 0)

    def axial(n):
        cycle = n // 2
        lanes = pl.ds(pl.multiple_of((n % 2) * 128, 128), 128)
        cells = [
            jnp.concatenate(
                [column[c, 4 + cycle, :, lanes], jnp.where(row8 < 4, z_high[c, cycle, :, lanes], z_low[c, cycle, :, lanes])], 0
            )
            for c in range(6)
        ]
        material = jnp.concatenate(
            [column_ph[4 + cycle, :, lanes], jnp.where(row8 < 4, z_high_ph[cycle, :, lanes], z_low_ph[cycle, :, lanes])], 0
        )
        inverse, pressure = primitives(cells, material == 1)
        velocity = cells[3] * inverse
        for c in range(6):
            upward, downward = split_flux(cells, velocity, pressure, 3, c)
            change = line_divergence(upward, downward, 0)[:32] * (0.5 * quarter)
            result[c, cycle, :, lanes] = result[c, cycle, :, lanes] - change

    def arrive_and_forward(k):
        @pl.when(forwards)
        def _():
            for copy in arrival(k, 3, x_recv):
                copy.wait_recv()

        @pl.when(jnp.logical_and(forwards, row > 0))
        def _():
            for copy in forward(k):
                copy.start()

        @pl.when(first)
        def _():
            for copy in forward_two(k):
                copy.start()

    def x_arrive(k):
        @pl.when(jnp.logical_not(forwards))
        def _():
            for copy in arrival(k, 3, x_recv):
                copy.wait_recv()

        @pl.when(jnp.logical_and(forwards, row > 0))
        def _():
            for copy in arrival(k, 1, b_recv):
                copy.wait_recv()

    def y_arrive(k):
        @pl.when(jnp.logical_and(row != 7, row != 2))
        def _():
            for copy in arrival(k, 3, y_recv):
                copy.wait_recv()

        @pl.when(row == 2)
        def _():
            for copy in arrival(k, 2, y_recv) + arrival(k, 1, c_recv):
                copy.wait_recv()

    flip = jnp.where(first, -1.0, 1.0)

    def radial(k):
        rows, lanes = piece(k)
        planes = [jnp.where(first, 4 - p, p) for p in (1, 2, 3)] + list(range(4, 11))
        stack = []
        for i, plane in enumerate(planes):
            cells = [column[c, plane, rows, lanes] for c in range(6)]
            if i < 3:
                cells[1] = cells[1] * flip
                cells[2] = cells[2] * flip
            inverse, pressure = primitives(cells, column_ph[plane, rows, lanes] == 1)
            stack.append((cells, cells[1] * inverse, pressure))
        for c in range(6):
            up, down = zip(*[split_flux(cells, v, p, 1, c) for cells, v, p in stack])

            def pieces(field):
                u = [field[i + 1] - field[i] for i in range(9)]
                d = [None] + [u[i] - u[i - 1] for i in range(1, 9)]
                q = [None] + [d[i] * d[i] + scaled_epsilon for i in range(1, 9)]
                return u, d, q

            u, d, q = pieces(up)
            right = [
                up[i] + correction(u[i - 2], u[i - 1], u[i], u[i + 1], d[i - 1], d[i], d[i + 1], q[i - 1], q[i], q[i + 1])
                for i in range(2, 7)
            ]
            u, d, q = pieces(down)
            left = [
                down[i] - correction(u[i + 1], u[i], u[i - 1], u[i - 2], -d[i + 1], -d[i], -d[i - 1], q[i + 1], q[i], q[i - 1])
                for i in range(3, 8)
            ]
            face = [a + b for a, b in zip(right, left)]
            weighted = [(row * 4 + j).astype(jnp.float32) * face[j] for j in range(5)]
            for j in range(4):
                radius = (row * 4 + j).astype(jnp.float32) + 0.5
                result[c, j, rows, lanes] = result[c, j, rows, lanes] - (weighted[j + 1] - weighted[j]) * (0.5 * quarter / radius)

    def axial_step(n, _):
        axial(n)
        return 0

    def azimuthal_steps(n, _):
        lax.fori_loop(2 * n, 2 * n + 2, azimuthal, 0)
        arrive_and_forward(n)
        return 0

    lax.fori_loop(0, 4, azimuthal_steps, 0)
    hand_over()
    for copy in z_copies():
        copy.wait_recv()

    def axial_steps(n, _):
        lax.fori_loop(2 * n, 2 * n + 2, axial_step, 0)

        @pl.when(jnp.logical_and(row > 0, n < 3))
        def _():
            arrive_and_forward(4 + n)

        return 0

    lax.fori_loop(0, 4, axial_steps, 0)

    @pl.when(row > 0)
    def _():
        arrive_and_forward(7)

    @pl.when(first)
    def _():
        arrive_and_forward(4)
        arrive_and_forward(5)

    @pl.when(last)
    def _():
        for copy in rims():
            copy.wait()

    def tile(o):
        return pl.ds(o * 8, 8) if isinstance(o, int) else pl.ds(pl.multiple_of(o * 8, 8), 8)

    def out_copy(o):
        return pltpu.make_async_copy(result.at[:, :, tile(o), :], out_hbm.at[:, :, tile(o), :], out_sem.at[o])

    mine = pl.multiple_of(lax.rem(theta, 2) * 96, 8)
    other = pl.multiple_of(96 - lax.rem(theta, 2) * 96, 8)

    def share(step, o, source, target, where):
        return pltpu.make_async_remote_copy(
            src_ref=source,
            dst_ref=target,
            send_sem=f_send.at[4 * step + o],
            recv_sem=f_recv.at[4 * step + o],
            device_id={"theta": where},
            device_id_type=MESH,
        )

    def step_one(o):
        return share(0, o, part.at[o, pl.ds(other, 96)], half_got.at[o], sibling)

    def step_two(o):
        return share(1, o, half_sum.at[o], half_far.at[o], theta_far)

    def step_three(o):
        return share(2, o, half_total.at[o], half_peer.at[o], sibling)

    def filter_one(o):
        values = result[:, :, tile(o), :].reshape(192, 256)
        part[o] = product(values, table, table_low)
        step_one(o).start()

    def filter_two(o):
        step_one(o).wait_recv()
        half_sum[o] = part[o, pl.ds(mine, 96)] + half_got[o]
        step_two(o).start()

    def filter_three(o):
        step_two(o).wait_recv()
        half_total[o] = half_sum[o] + half_far[o]
        step_three(o).start()

    def filter_last(o, _):
        order = lax.broadcasted_iota(jnp.int32, (8, 128), 1)
        order = jnp.where(order < KMODES, order, order - KMODES)
        mode_scale = jnp.where(order == 0, 1.0 / NT, 2.0 / NT)
        weights = [jnp.where(order <= cutoff_smem[i], mode_scale, 0.0) for i in range(4)]
        weights = jnp.concatenate(weights * 3, 0)
        even_core = lax.rem(theta, 2) == 0
        step_three(o).wait_recv()
        own = half_total[o] * weights
        peer = half_peer[o] * weights
        lower = jnp.where(even_core, own, peer)
        upper = jnp.where(even_core, peer, own)
        coefficients = jnp.concatenate([lower, upper], 0)
        values = product(coefficients, table_t, table_t_low)
        result[:, :, tile(o), :] = values.reshape(6, 4, 8, 256)
        out_copy(o).start()
        return 0

    @pl.when(first)
    def _():
        for copy in table_loads():
            copy.wait()

    def radial_step(k, _):
        @pl.when(jnp.logical_and(first, k == 2))
        def _():
            arrive_and_forward(6)

        @pl.when(jnp.logical_and(first, k == 5))
        def _():
            arrive_and_forward(7)

        @pl.when(jnp.logical_and(first, jnp.logical_and(k > 4, k < 5 + ASIDE)))
        def _():
            for copy in arrival(k - 5, 1, b_recv):
                copy.wait_recv()
            for copy in forward_fourth(k - 5):
                copy.start()

        x_arrive(k)
        y_arrive(k)
        radial(k)
        o = k // 2
        whole = lax.rem(k, 2) == 1

        @pl.when(jnp.logical_and(whole, first))
        def _():
            @pl.when(o > 0)
            def _():
                filter_two(o - 1)

            filter_one(o)

        @pl.when(jnp.logical_and(whole, jnp.logical_not(first)))
        def _():
            out_copy(o).start()

        return 0

    lax.fori_loop(0, 8, radial_step, 0)

    @pl.when(first)
    def _():
        filter_two(3)
        for o in range(3):
            filter_three(o)
        lax.fori_loop(0, 2, filter_last, 0)
        filter_three(3)
        lax.fori_loop(2, 4, filter_last, 0)
        for k in range(ASIDE):
            for copy in forward_fourth(k):
                copy.wait_send()
        for o in range(4):
            step_one(o).wait_send()
            step_two(o).wait_send()
            step_three(o).wait_send()

    for copy in t_copies():
        copy.wait_send()
    for copy in z_copies():
        copy.wait_send()
    for k in range(8):
        for copy in x_first(k):
            copy.wait_send()

        @pl.when(inner_row)
        def _():
            for copy in x_fourth(k):
                copy.wait_send()

        @pl.when(first)
        def _():
            for copy in mirror(k) + forward_two(k):
                copy.wait_send()

        @pl.when(jnp.logical_and(forwards, row > 0))
        def _():
            for copy in forward(k):
                copy.wait_send()

    @pl.when(row == 1)
    def _():
        for k in range(DIRECT, 8):
            for copy in relay_on(k):
                copy.wait_send()

    @pl.when(row == 3)
    def _():
        for k in range(ASIDE, 8):
            for copy in fourth_on(k):
                copy.wait_send()

    for o in range(4):
        out_copy(o).wait()


def fourier_tables():
    phases = (np.arange(NT)[:, None] * np.arange(KMODES)[None, :]) % NT
    angles = phases.astype(np.float64) * (2.0 * np.pi / NT)
    table = np.concatenate([np.cos(angles), np.sin(angles)], 1).astype(np.float32).reshape(4, 256, 2 * KMODES)
    halves = []
    for matrix in (table, np.ascontiguousarray(table.transpose(0, 2, 1))):
        high = matrix.astype(jnp.bfloat16)
        halves += [high, (matrix - high.astype(np.float32)).astype(jnp.bfloat16)]
    return halves


def shards(state_start, state_section, phase, cutoff):
    f32, i32 = jnp.float32, jnp.int32
    tables = [jnp.asarray(matrix) for matrix in fourier_tables()]
    anywhere = pl.BlockSpec(memory_space=pltpu.HBM)
    dma = pltpu.SemaphoreType.DMA
    return pl.pallas_call(
        kernel,
        out_shape=jax.ShapeDtypeStruct(state_start.shape, f32),
        in_specs=[anywhere] * 8,
        out_specs=anywhere,
        scratch_shapes=[
            pltpu.VMEM((6, 12, 32, 256), f32),
            pltpu.VMEM((12, 32, 256), i32),
            pltpu.VMEM((6, 4, 32, 256), f32),
            pltpu.VMEM((6, 4, 8, 256), f32),
            pltpu.VMEM((4, 8, 256), i32),
            pltpu.VMEM((6, 4, 8, 256), f32),
            pltpu.VMEM((4, 8, 256), i32),
            pltpu.VMEM((32, 128), f32),
            pltpu.VMEM((32, 128), f32),
            pltpu.VMEM((32, 128), f32),
            pltpu.VMEM((32, 128), f32),
            pltpu.VMEM((256, 2 * KMODES), jnp.bfloat16),
            pltpu.VMEM((256, 2 * KMODES), jnp.bfloat16),
            pltpu.VMEM((2 * KMODES, 256), jnp.bfloat16),
            pltpu.VMEM((2 * KMODES, 256), jnp.bfloat16),
            pltpu.VMEM((4, 192, 2 * KMODES), f32),
            pltpu.VMEM((4, 96, 2 * KMODES), f32),
            pltpu.VMEM((4, 96, 2 * KMODES), f32),
            pltpu.VMEM((4, 96, 2 * KMODES), f32),
            pltpu.VMEM((4, 96, 2 * KMODES), f32),
            pltpu.VMEM((4, 96, 2 * KMODES), f32),
            pltpu.VMEM((6, 3, 32, 256), f32),
            pltpu.VMEM((3, 32, 256), i32),
            pltpu.SMEM((4,), i32),
            dma((8,)),
            dma((8,)),
            dma((6,)),
            dma((6,)),
            *[dma((16,))] * 10,
            dma((4,)),
            dma((4,)),
            dma((2,)),
            dma((2,)),
            dma((12,)),
            dma((12,)),
            dma((4,)),
        ],
        compiler_params=pltpu.CompilerParams(collective_id=0, has_side_effects=True, vmem_limit_bytes=67043328),
        name="jet_section",
    )(state_start, state_section, phase, cutoff, *tables)


def solution(mesh):
    in_specs = (
        P(None, "row", "gz", "theta"),
        P(None, "row", "gz", "theta"),
        P("row", "gz", "theta"),
        P(),
    )
    out_specs = P(None, "row", "gz", "theta")
    return jax.shard_map(shards, mesh=mesh, in_specs=in_specs, out_specs=out_specs, check_vma=False)
```
